8 devices in a mesh: rep: 2 (over z, y), dp: 4 (over x, core).
Axes of the slice: x: 2, y: 2, z: 1, core: 2. Of those that a mesh axis runs over, the one named last changes fastest.
Arguments:
- hidden: bfloat16 [256, 2048], P(('rep', 'dp')), parts along dimension 0
- lengths: int32 [256], P(('rep', 'dp')), parts along dimension 0
- kv_cache: bfloat16 [2, 256, 128, 576], P(None, ('rep', 'dp')), parts along dimension 1
- norm_attn: float32 [2, 2048], replicated
- w_q: bfloat16 [2, 2048, 9216], replicated
- w_o: bfloat16 [2, 8192, 2048], replicated
- norm_ffn: float32 [2, 2048], replicated
- w_gate: bfloat16 [2, 2048, 10944], P(None, None, 'dp')
- w_up: bfloat16 [2, 2048, 10944], P(None, None, 'dp')
- w_down: bfloat16 [2, 10944, 2048], P(None, 'dp')
- norm_final: float32 [2048], replicated
- w_head: bfloat16 [2048, 102400], P(None, 'dp')
Outputs:
- output: float32 [256, 102400], P('rep', 'dp'), parts along dimension 0
There are 2 independent parts. The reference program is written for one: setup_inputs(seed, part) draws one part's arguments, and reference() takes and returns one part's arrays. A program takes and returns all parts, laid end to end along the dimension named above; an argument that names none is the same for every part.
All inputs are finite; a program needn't handle non-finite values.
Results may differ from the reference program's by a relative error of at most 0.02.
Values are sent between devices in bfloat16 or wider.
A program may use at most 1.5 GiB of HBM per device.

```python
import jax
import jax.numpy as jnp
from jax import lax

BATCH_SIZE = 128
SEQ_LEN = 128
D_MODEL = 2048
NUM_HEADS = 16
FFN_DIM = 10944
VOCAB_SIZE = 102400
NUM_LAYERS = 2
LATENT_DIM = 512
ROPE_DIM = 64
KV_WIDTH = LATENT_DIM + ROPE_DIM
QK_SCALE = 192 ** -0.5
NORM_EPS = 1e-6


def setup_inputs(seed: int = 0, part: int = 0) -> dict:
    own_keys = jax.random.split(jax.random.fold_in(jax.random.key(seed), part), 3)
    shared_keys = jax.random.split(jax.random.key(seed + 1), 9)
    hidden = jax.random.normal(own_keys[0], (BATCH_SIZE, D_MODEL), jnp.float32)
    lengths = jax.random.randint(own_keys[1], (BATCH_SIZE,), 1, SEQ_LEN + 1, jnp.int32)
    lengths = lengths.at[0].set(SEQ_LEN)
    kv_cache = jax.random.normal(own_keys[2], (NUM_LAYERS, BATCH_SIZE, SEQ_LEN, KV_WIDTH), jnp.float32)
    attn_gain = SEQ_LEN ** 0.5 / 8.0
    norm_attn = jax.random.uniform(shared_keys[0], (NUM_LAYERS, D_MODEL), jnp.float32, 0.5, 1.5)
    w_q = jax.random.normal(shared_keys[1], (NUM_LAYERS, D_MODEL, NUM_HEADS * KV_WIDTH), jnp.float32) * D_MODEL ** -0.5
    w_o = jax.random.normal(shared_keys[2], (NUM_LAYERS, NUM_HEADS * LATENT_DIM, D_MODEL), jnp.float32) * ((NUM_HEADS * LATENT_DIM) ** -0.5 * attn_gain)
    norm_ffn = jax.random.uniform(shared_keys[3], (NUM_LAYERS, D_MODEL), jnp.float32, 0.5, 1.5)
    w_gate = jax.random.normal(shared_keys[4], (NUM_LAYERS, D_MODEL, FFN_DIM), jnp.float32) * D_MODEL ** -0.5
    w_up = jax.random.normal(shared_keys[5], (NUM_LAYERS, D_MODEL, FFN_DIM), jnp.float32) * D_MODEL ** -0.5
    w_down = jax.random.normal(shared_keys[6], (NUM_LAYERS, FFN_DIM, D_MODEL), jnp.float32) * (2.0 * FFN_DIM ** -0.5)
    norm_final = jax.random.uniform(shared_keys[7], (D_MODEL,), jnp.float32, 0.5, 1.5)
    w_head = jax.random.normal(shared_keys[8], (D_MODEL, VOCAB_SIZE), jnp.float32) * D_MODEL ** -0.5
    return dict(
        hidden=hidden.astype(jnp.bfloat16),
        lengths=lengths,
        kv_cache=kv_cache.astype(jnp.bfloat16),
        norm_attn=norm_attn,
        w_q=w_q.astype(jnp.bfloat16),
        w_o=w_o.astype(jnp.bfloat16),
        norm_ffn=norm_ffn,
        w_gate=w_gate.astype(jnp.bfloat16),
        w_up=w_up.astype(jnp.bfloat16),
        w_down=w_down.astype(jnp.bfloat16),
        norm_final=norm_final,
        w_head=w_head.astype(jnp.bfloat16),
    )


def rms_norm(x_rows, gain_vec):
    x_float = x_rows.astype(jnp.float32)
    inv_rms = lax.rsqrt(jnp.mean(x_float * x_float, axis=-1, keepdims=True) + NORM_EPS)
    return (x_float * inv_rms * gain_vec).astype(jnp.bfloat16)


def attend_row(row_args):
    q_heads, cache_row, length = row_args
    cache_float = cache_row.astype(jnp.float32)
    scores = jnp.dot(q_heads.astype(jnp.float32), cache_float.T, preferred_element_type=jnp.float32) * QK_SCALE
    key_valid = jnp.arange(cache_row.shape[0]) < length
    scores = jnp.where(key_valid[None, :], scores, -1e30)
    attn_probs = jax.nn.softmax(scores, axis=-1).astype(jnp.bfloat16)
    context = jnp.dot(attn_probs.astype(jnp.float32), cache_float[:, :LATENT_DIM], preferred_element_type=jnp.float32)
    return context.astype(jnp.bfloat16)


def reference(hidden, lengths, kv_cache, norm_attn, w_q, w_o, norm_ffn, w_gate, w_up, w_down, norm_final, w_head):
    num_rows = hidden.shape[0]

    def layer_step(x_rows, layer_args):
        layer_cache, attn_norm, wq_layer, wo_layer, ffn_norm, gate_layer, up_layer, down_layer = layer_args
        normed = rms_norm(x_rows, attn_norm)
        q_all = jnp.dot(normed, wq_layer, preferred_element_type=jnp.float32).astype(jnp.bfloat16)
        q_all = q_all.reshape(num_rows, NUM_HEADS, KV_WIDTH)
        context = lax.map(attend_row, (q_all, layer_cache, lengths)).reshape(num_rows, NUM_HEADS * LATENT_DIM)
        x_rows = (x_rows.astype(jnp.float32) + jnp.dot(context, wo_layer, preferred_element_type=jnp.float32)).astype(jnp.bfloat16)
        normed = rms_norm(x_rows, ffn_norm)
        gate_proj = jnp.dot(normed, gate_layer, preferred_element_type=jnp.float32)
        up_proj = jnp.dot(normed, up_layer, preferred_element_type=jnp.float32)
        act_rows = (jax.nn.silu(gate_proj) * up_proj).astype(jnp.bfloat16)
        ffn_out = jnp.dot(act_rows, down_layer, preferred_element_type=jnp.float32)
        x_rows = (x_rows.astype(jnp.float32) + ffn_out).astype(jnp.bfloat16)
        return x_rows, None

    layer_inputs = (kv_cache, norm_attn, w_q, w_o, norm_ffn, w_gate, w_up, w_down)
    x_final, layer_outs = lax.scan(layer_step, hidden, layer_inputs)
    normed = rms_norm(x_final, norm_final)
    return jnp.dot(normed, w_head, preferred_element_type=jnp.float32)
```

```python
import functools

import jax
import jax.numpy as jnp
from jax import lax
from jax.experimental import pallas as pl
from jax.experimental.pallas import tpu as pltpu
from jax.sharding import PartitionSpec as P

F32 = jnp.float32
BF16 = jnp.bfloat16
MESH = pl.DeviceIdType.MESH

D = 2048
HEADS = 16
LATENT = 512
KV_W = 576
SEQ = 128
ROWS = 32
CHIP = 64
ALL = 128
FFN = 2736
FFN_PAD = 2816
NC = 512
QH = HEADS * KV_W // 2
PAIR = 2 * KV_W
VOCAB = 25600
QK_SCALE = 192 ** -0.5
NORM_EPS = 1e-6
LAYERS = 2


def _rows_norm(chunks, gain, dtype=BF16):
    ss = sum(jnp.sum(v * v, axis=-1, keepdims=True) for v in chunks)
    inv = lax.rsqrt(ss * (1.0 / D) + NORM_EPS)
    return [(v * inv * gain[:, i * NC:(i + 1) * NC]).astype(dtype) for i, v in enumerate(chunks)]


def body(hid_h, lens_h, ga_h, gf_h, gl_h, kv, wq, wo, wg, wu, wd, wh, H, S, G, DN,
         hid, lens, ga, gf, gl, in_sem, KV, X, Qf, Qs, O16, A, PS, CS, R1, R2,
         s_sem, g_sem, d_sem, kv_sem, q_ss, q_rs, o_ss, o_rs, ad_ss, ad_rs, al_ss, al_rs, af_ss, af_rs,
         p_ss, p_rs, c_ss, c_rs, h_ss, h_rs):
    me = lax.axis_index('dp')
    c = lax.rem(me, 2)
    chip = me // 2
    partner = me + 1 - 2 * c
    other = lax.rem(me + 2, 4)
    my_row = pl.multiple_of(me * ROWS, ROWS)
    pa_row = pl.multiple_of(partner * ROWS, ROWS)
    chip_row = pl.multiple_of(chip * CHIP, CHIP)
    oth_row = pl.multiple_of((1 - chip) * CHIP, CHIP)

    def rdma(src, dst, ss, rs, dev):
        return pltpu.make_async_remote_copy(src_ref=src, dst_ref=dst, send_sem=ss, recv_sem=rs,
                                            device_id={'dp': dev}, device_id_type=MESH)

    def cp_wq(l, i):
        p, kk = i // 2, i % 2
        col = pl.multiple_of(c * QH + p * PAIR, 128)
        return pltpu.make_async_copy(wq.at[l, pl.ds(kk * 1024, 1024), pl.ds(col, PAIR)], S.at[i], s_sem.at[i])

    def cp_wo(l, i):
        col = pl.multiple_of(c * 1024, 128)
        return pltpu.make_async_copy(wo.at[l, pl.ds(i * 1024, 1024), pl.ds(col, 1024)],
                                     S.at[i, :, pl.ds(0, 1024)], s_sem.at[i])

    def cp_g(l, i):
        w, j = i // 6, i % 6
        src = wg if w == 0 else wu
        return pltpu.make_async_copy(src.at[l, pl.ds(j * 456, 456), :], G.at[w, pl.ds(j * 456, 456), :], g_sem.at[i])

    def dn_col(i):
        owner = 1 - c if i % 2 == 0 else c
        return 2 * owner + i // 2

    def cp_d(l, i):
        col = pl.multiple_of(dn_col(i) * NC, NC)
        return pltpu.make_async_copy(wd.at[l, :, pl.ds(col, NC)], DN.at[i, pl.ds(0, FFN), :], d_sem.at[i])

    def cp_kv(l, i):
        return pltpu.make_async_copy(kv.at[l, pl.ds(i * 8, 8)], KV.at[pl.ds(i * 8, 8)], kv_sem.at[i])

    def cp_hs(i):
        return pltpu.make_async_copy(wh.at[pl.ds((i % 2) * 1024, 1024), pl.ds((i // 2) * 1024, 1024)],
                                     S.at[i, :, pl.ds(0, 1024)], s_sem.at[i])

    def cp_hg(i):
        g, j = i // 4, i % 4
        return pltpu.make_async_copy(wh.at[pl.ds(j * 512, 512), pl.ds(4096 + g * D, D)],
                                     G.at[g, pl.ds(j * 512, 512), :], g_sem.at[i])

    def cp_hd(i):
        return pltpu.make_async_copy(wh.at[:, pl.ds(8192 + i * NC, NC)], DN.at[i, pl.ds(0, D), :], d_sem.at[i])

    ins = [pltpu.make_async_copy(a, b, in_sem.at[i]) for i, (a, b) in enumerate(
        ((hid_h, hid), (lens_h, lens), (ga_h, ga), (gf_h, gf), (gl_h, gl)))]
    for cp in ins:
        cp.start()
    for i in range(4):
        cp_wq(0, i).start()

    bar = pltpu.get_barrier_semaphore()
    for dev in (partner, other):
        pl.semaphore_signal(bar, inc=1, device_id={'dp': dev}, device_id_type=MESH)
    pl.semaphore_wait(bar, 2)

    ins[0].wait()
    for n in range(4):
        X[n, pl.ds(my_row, ROWS), :] = hid[:, n * NC:(n + 1) * NC]
    hx = rdma(X.at[:, pl.ds(my_row, ROWS), :], X.at[:, pl.ds(my_row, ROWS), :], h_ss.at[0], h_rs.at[0], partner)
    hx.start()
    for i in range(4):
        DN[i, FFN:FFN_PAD, :] = jnp.zeros((FFN_PAD - FFN, NC), BF16)
    A[:, FFN_PAD - 128:FFN_PAD] = jnp.zeros((ALL, 128), BF16)
    for cp in ins[1:]:
        cp.wait()
    hx.wait_send()
    rdma(X.at[:, pl.ds(pa_row, ROWS), :], X.at[:, pl.ds(pa_row, ROWS), :], h_ss.at[0], h_rs.at[0], partner).wait_recv()

    def x_chunks(row, rows):
        return [X[n, pl.ds(row, rows), :].astype(F32) for n in range(4)]

    def norm_to_h(row, rows, h_row, gain):
        for n, v in enumerate(_rows_norm(x_chunks(row, rows), gain)):
            H[pl.ds(h_row, rows), n * NC:(n + 1) * NC] = v

    def own_n(j):
        return 2 * c + j

    def par_n(j):
        return 2 * (1 - c) + j

    def ad(j, n):
        r = X.at[n, pl.ds(chip_row, CHIP), :]
        return rdma(r, r, ad_ss.at[j], ad_rs.at[j], partner)

    def al(j, row):
        r = X.at[own_n(j), pl.ds(row, CHIP), :]
        return rdma(r, r, al_ss.at[j], al_rs.at[j], other)

    def af(j, n):
        r = X.at[n, pl.ds(oth_row, CHIP), :]
        return rdma(r, r, af_ss.at[j], af_rs.at[j], partner)

    def gather_start(j):
        al(j, chip_row).start()
        ad(j, own_n(j)).start()

    def gather_finish():
        for j in range(2):
            al(j, oth_row).wait_recv()
            af(j, own_n(j)).start()
        for j in range(2):
            ad(j, par_n(j)).wait_recv()
        for j in range(2):
            af(j, par_n(j)).wait_recv()
        for j in range(2):
            al(j, chip_row).wait_send()
            ad(j, own_n(j)).wait_send()
            af(j, own_n(j)).wait_send()

    for l in range(LAYERS):
        norm_to_h(my_row, ROWS, 0, ga[l:l + 1, :])
        norm_to_h(pa_row, ROWS, ROWS, ga[l:l + 1, :])

        def q_send(p):
            dst = Qf.at[:, pl.ds(pl.multiple_of((c * 8 + 2 * p) * ROWS, ROWS), 2 * ROWS), :]
            return rdma(Qs.at[:, pl.ds(2 * p * ROWS, 2 * ROWS), :], dst, q_ss.at[p], q_rs.at[p], partner)

        def q_recv(p):
            dst = Qf.at[:, pl.ds(pl.multiple_of(((1 - c) * 8 + 2 * p) * ROWS, ROWS), 2 * ROWS), :]
            return rdma(dst, dst, q_ss.at[p], q_rs.at[p], partner)

        for p in range(4):
            cp_wq(l, 2 * p).wait()
            cp_wq(l, 2 * p + 1).wait()
            if l == 0:
                if p < 2:
                    cp_wq(0, 2 * p + 4).start()
                    cp_wq(0, 2 * p + 5).start()
                if p == 1:
                    for i in range(4):
                        cp_kv(0, i).start()
                if p == 2:
                    for i in range(4):
                        cp_wo(0, i).start()
            r = jnp.dot(H[0:CHIP, 0:1024], S[2 * p], preferred_element_type=F32)
            r = r + jnp.dot(H[0:CHIP, 1024:2048], S[2 * p + 1], preferred_element_type=F32)
            if l > 0 or p > 1:
                cp_wo(l, 2 * p).start()
                cp_wo(l, 2 * p + 1).start()
            r = r.astype(BF16).astype(F32)
            for j in range(2):
                rj = r[:, j * KV_W:(j + 1) * KV_W]
                row = pl.multiple_of((c * 8 + 2 * p + j) * ROWS, ROWS)
                rj = jnp.concatenate([rj, jnp.zeros((CHIP, 64), F32)], axis=1)
                for t in range(5):
                    v = rj[:, t * 128:(t + 1) * 128]
                    Qf[t, pl.ds(row, ROWS), :] = v[0:ROWS]
                    Qs[t, (2 * p + j) * ROWS:(2 * p + j + 1) * ROWS, :] = v[ROWS:CHIP]
            q_send(p).start()
        for p in range(4):
            q_recv(p).wait_recv()
        for p in range(4):
            q_send(p).wait_send()

        def o_send(g2):
            r0 = g2 * 16
            return rdma(O16.at[:, pl.ds(r0, 16), :], O16.at[:, pl.ds(ROWS + r0, 16), :],
                        o_ss.at[g2], o_rs.at[g2], partner)

        for g in range(4):
            cp_kv(l, g).wait()
            if l == 0 and g > 0:
                for i in range(4):
                    cp_g(0, 4 * (g - 1) + i).start()
            sc = []
            for i in range(8):
                b = g * 8 + i
                qb = jnp.concatenate([Qf[t, pl.ds(b, HEADS, stride=ROWS), :] for t in range(5)], axis=1)
                s = jnp.dot(qb[:, 0:KV_W].astype(BF16), KV[b], preferred_element_type=F32) * QK_SCALE
                pos = lax.broadcasted_iota(jnp.int32, (HEADS, SEQ), 1)
                sc.append(jnp.where(pos < lens[b], s, -1e30))
            s = jnp.concatenate(sc, axis=0)
            e = jnp.exp(s - jnp.max(s, axis=-1, keepdims=True))
            pr = (e / jnp.sum(e, axis=-1, keepdims=True)).astype(BF16)
            for i in range(8):
                b = g * 8 + i
                o = lax.dot_general(pr[i * HEADS:(i + 1) * HEADS], KV[b, 0:LATENT, :], (((1,), (1,)), ((), ())),
                                    preferred_element_type=F32)
                for t in range(4):
                    Qf[t, pl.ds(b, HEADS, stride=ROWS), :] = o[:, t * 128:(t + 1) * 128]
            if g % 2 == 1:
                r0 = (g // 2) * 16
                for h in range(HEADS):
                    for t in range(4):
                        O16[h, r0:r0 + 16, t * 128:(t + 1) * 128] = (
                            Qf[t, h * ROWS + r0:h * ROWS + r0 + 16, :].astype(BF16))
                o_send(g // 2).start()
        for g2 in range(2):
            r0 = g2 * 16
            ref = O16.at[:, pl.ds(ROWS + r0, 16), :]
            rdma(ref, ref, o_ss.at[g2], o_rs.at[g2], partner).wait_recv()
        for g2 in range(2):
            o_send(g2).wait_send()

        for i in range(8):
            cp_wo(l, i).wait()
        if l == 0:
            for i in range(4):
                cp_d(0, i).start()
        for j in range(2):
            acc = None
            for k in range(8):
                for hh in range(2):
                    t = jnp.dot(O16[2 * k + hh], S[k, hh * LATENT:(hh + 1) * LATENT, j * NC:(j + 1) * NC],
                                preferred_element_type=F32)
                    acc = t if acc is None else acc + t
            n = own_n(j)
            X[n, pl.ds(my_row, ROWS), :] = (X[n, pl.ds(my_row, ROWS), :].astype(F32) + acc[0:ROWS]).astype(BF16)
            X[n, pl.ds(pa_row, ROWS), :] = (X[n, pl.ds(pa_row, ROWS), :].astype(F32) + acc[ROWS:CHIP]).astype(BF16)
            gather_start(j)
        if l + 1 == LAYERS:
            for i in range(8):
                cp_hs(i).start()
        gather_finish()

        for r in range(4):
            norm_to_h(r * ROWS, ROWS, r * ROWS, gf[l:l + 1, :])
        if l + 1 < LAYERS:
            for i in range(8):
                cp_wq(l + 1, i).start()
            for i in range(4):
                cp_kv(l + 1, i).start()
        for i in range(12):
            cp_g(l, i).wait()

        def ffn_cols(n0, size):
            g_ = lax.dot_general(H[...], G[0, pl.ds(n0, size), :], (((1,), (1,)), ((), ())),
                                 preferred_element_type=F32)
            u_ = lax.dot_general(H[...], G[1, pl.ds(n0, size), :], (((1,), (1,)), ((), ())),
                                 preferred_element_type=F32)
            A[:, pl.ds(n0, size)] = (jax.nn.silu(g_) * u_).astype(BF16)

        def ffn_step(n, carry):
            ffn_cols(pl.multiple_of(n * NC, NC), NC)
            return carry

        lax.fori_loop(0, 5, ffn_step, 0)
        ffn_cols(5 * NC, FFN - 5 * NC)
        if l + 1 < LAYERS:
            for i in range(12):
                cp_g(l + 1, i).start()
        else:
            for i in range(8):
                cp_hg(i).start()

        def ps(j):
            return rdma(PS.at[j], R1.at[j], p_ss.at[j], p_rs.at[j], partner)

        def cs(j):
            return rdma(CS.at[j, pl.ds(oth_row, CHIP), :], R2.at[j], c_ss.at[j], c_rs.at[j], other)

        def down(i):
            cp_d(l, i).wait()
            y = jnp.dot(A[...], DN[i], preferred_element_type=F32)
            if l + 1 < LAYERS:
                cp_d(l + 1, i).start()
            else:
                cp_hd(i).start()
            return y

        def chip_sum(j):
            ps(j).wait_recv()
            CS[j] = CS[j] + R1[j]
            cs(j).start()

        PS[0] = down(0)
        ps(0).start()
        CS[0] = down(1)
        PS[1] = down(2)
        ps(1).start()
        chip_sum(0)
        CS[1] = down(3)
        chip_sum(1)
        last = l + 1 == LAYERS
        for j in range(2):
            cs(j).wait_recv()
            n = own_n(j)
            xr = X[n, pl.ds(chip_row, CHIP), :].astype(F32)
            X[n, pl.ds(chip_row, CHIP), :] = (xr + (CS[j, pl.ds(chip_row, CHIP), :] + R2[j])).astype(BF16)
            if last:
                gather_start(j)
            else:
                ad(j, own_n(j)).start()
        for j in range(2):
            ps(j).wait_send()
            cs(j).wait_send()
        if last:
            gather_finish()
        else:
            for j in range(2):
                ad(j, par_n(j)).wait_recv()
            for j in range(2):
                ad(j, own_n(j)).wait_send()

    for r in range(4):
        norm_to_h(r * ROWS, ROWS, r * ROWS, gl[...])
    for i in range(8):
        cp_hs(i).wait()
        cp_hg(i).wait()
    for i in range(4):
        cp_hd(i).wait()


RING = 4
BLOCKS = VOCAB // NC
HELD = 20
STREAM = BLOCKS - HELD


def head_body(H, S, G, DN, wh, out, W, OH, OS, w_sem, oh_sem, os_sem):
    def cp_w(t, slot):
        col = pl.multiple_of((HELD + t) * NC, NC)
        return pltpu.make_async_copy(wh.at[:, pl.ds(col, NC)], W.at[slot], w_sem.at[slot])

    def cp_out(buf, sems, block, slot):
        col = pl.multiple_of(block * NC, NC)
        return pltpu.make_async_copy(buf.at[slot], out.at[:, pl.ds(col, NC)], sems.at[slot])

    for t in range(RING):
        cp_w(t, t).start()

    def stream(t):
        slot, o = lax.rem(t, RING), lax.rem(t, 2)
        cp_w(t, slot).wait()

        @pl.when(t >= 2)
        def _():
            cp_out(OS, os_sem, HELD + t, o).wait()

        OS[o] = jnp.dot(H[...], W[slot], preferred_element_type=F32)
        cp_out(OS, os_sem, HELD + t, o).start()

        @pl.when(t + RING < STREAM)
        def _():
            cp_w(t + RING, slot).start()

    def held(t, value):
        o = lax.rem(t, 2)

        @pl.when(t >= 2)
        def _():
            cp_out(OH, oh_sem, t, o).wait()

        OH[o] = value()
        cp_out(OH, oh_sem, t, o).start()

    def dot(a, b):
        return jnp.dot(a, b, preferred_element_type=F32)

    def seg_s(t, carry):
        p, col = t // 2, pl.multiple_of(lax.rem(t, 2) * NC, NC)
        held(t, lambda: dot(H[:, 0:1024], S[2 * p, :, pl.ds(col, NC)])
             + dot(H[:, 1024:2048], S[2 * p + 1, :, pl.ds(col, NC)]))
        stream(t)
        return carry

    def seg_g(t, carry):
        g, col = t // 4 - 2, pl.multiple_of(lax.rem(t, 4) * NC, NC)
        held(t, lambda: dot(H[...], G[g, 0:D, pl.ds(col, NC)]))
        stream(t)
        return carry

    def seg_d(t, carry):
        held(t, lambda: dot(H[...], DN[t - 16, 0:D, :]))
        stream(t)
        return carry

    def seg_w(t, carry):
        stream(t)
        return carry

    lax.fori_loop(0, 8, seg_s, 0)
    lax.fori_loop(8, 16, seg_g, 0)
    lax.fori_loop(16, 20, seg_d, 0)
    lax.fori_loop(20, STREAM, seg_w, 0)
    for o in range(2):
        cp_out(OH, oh_sem, HELD - 2 + o, o).wait()
        cp_out(OS, os_sem, BLOCKS - 2 + o, o).wait()


def head_kernel(normed, s_buf, g_buf, d_buf, w_head):
    vm = pl.BlockSpec(memory_space=pltpu.VMEM)
    hb = pl.BlockSpec(memory_space=pl.ANY)
    dma = pltpu.SemaphoreType.DMA
    held = [pltpu.with_memory_space_constraint(a, pltpu.VMEM) for a in (normed, s_buf, g_buf, d_buf)]
    return pl.pallas_call(
        head_body,
        out_shape=jax.ShapeDtypeStruct((ALL, VOCAB), F32),
        in_specs=[vm] * 4 + [hb],
        out_specs=hb,
        scratch_shapes=[pltpu.VMEM((RING, D, NC), BF16), pltpu.VMEM((2, ALL, NC), F32), pltpu.VMEM((2, ALL, NC), F32),
                        dma((RING,)), dma((2,)), dma((2,))],
        compiler_params=pltpu.CompilerParams(vmem_limit_bytes=13500000),
        name='head',
    )(*held, w_head)


def layers_kernel(hidden, lengths, kv_t, norm_attn, w_q, w_o, norm_ffn, wg_t, wu_t, w_down, norm_final, w_head):
    hb = pl.BlockSpec(memory_space=pl.ANY)
    dma = pltpu.SemaphoreType.DMA
    vm = pl.BlockSpec(memory_space=pltpu.VMEM)
    scratch = [
        pltpu.VMEM((ROWS, D), BF16), pltpu.SMEM((ROWS,), jnp.int32), pltpu.VMEM((2, D), F32), pltpu.VMEM((2, D), F32),
        pltpu.VMEM((1, D), F32), dma((5,)),
        pltpu.VMEM((ROWS, KV_W, SEQ), BF16),
        pltpu.VMEM((4, ALL, NC), BF16),
        pltpu.VMEM((5, HEADS * ROWS, 128), F32),
        pltpu.VMEM((5, 8 * ROWS, 128), F32),
        pltpu.VMEM((HEADS, CHIP, LATENT), BF16),
        pltpu.VMEM((ALL, FFN_PAD), BF16),
        pltpu.VMEM((2, ALL, NC), F32),
        pltpu.VMEM((2, ALL, NC), F32),
        pltpu.VMEM((2, ALL, NC), F32),
        pltpu.VMEM((2, CHIP, NC), F32),
        dma((8,)), dma((12,)), dma((4,)), dma((4,)),
        dma((4,)), dma((4,)), dma((2,)), dma((2,)),
        dma((2,)), dma((2,)), dma((2,)), dma((2,)), dma((2,)), dma((2,)),
        dma((2,)), dma((2,)), dma((2,)), dma((2,)), dma((1,)), dma((1,)),
    ]
    return pl.pallas_call(
        body,
        out_shape=[pltpu.VMEM((ALL, D), BF16), pltpu.VMEM((8, 1024, PAIR), BF16), pltpu.VMEM((2, FFN, D), BF16),
                   pltpu.VMEM((4, FFN_PAD, NC), BF16)],
        in_specs=[hb] * 12,
        out_specs=[vm] * 4,
        scratch_shapes=scratch,
        compiler_params=pltpu.CompilerParams(collective_id=0, has_side_effects=True, vmem_limit_bytes=13500000),
        name='layers',
    )(hidden, lengths, norm_attn, norm_ffn, norm_final.reshape(1, D), kv_t, w_q, w_o, wg_t, wu_t, w_down, w_head)


def solution(mesh):
    row_axes = ('rep', 'dp')
    specs_in = (P(row_axes, None), P(row_axes), P(None, row_axes, None, None), P(), P(), P(), P(),
                P(None, None, 'dp'), P(None, None, 'dp'), P(None, 'dp', None), P(), P(None, 'dp'))

    def device_step(hidden, lengths, kv_cache, norm_attn, w_q, w_o, norm_ffn, w_gate, w_up, w_down, norm_final, w_head):
        held = layers_kernel(hidden, lengths, jnp.swapaxes(kv_cache, 2, 3), norm_attn, w_q, w_o, norm_ffn,
                               jnp.swapaxes(w_gate, 1, 2), jnp.swapaxes(w_up, 1, 2), w_down, norm_final, w_head)
        return head_kernel(*held, w_head)

    return jax.shard_map(device_step, mesh=mesh, in_specs=specs_in, out_specs=P('rep', 'dp'), check_vma=False)
```

```python
import functools

import jax
import jax.numpy as jnp
from jax import lax
from jax.experimental import pallas as pl
from jax.experimental.pallas import tpu as pltpu
from jax.sharding import PartitionSpec as P

F32 = jnp.float32
BF16 = jnp.bfloat16
MESH = pl.DeviceIdType.MESH

D = 2048
HEADS = 16
LATENT = 512
KV_W = 576
SEQ = 128
ROWS = 32
CHIP = 64
ALL = 128
FFN = 2736
FFN_PAD = 2816
NC = 512
QH = HEADS * KV_W // 2
PAIR = 2 * KV_W
VOCAB = 25600
QK_SCALE = 192 ** -0.5
NORM_EPS = 1e-6
LAYERS = 2


def _rows_norm(chunks, gain, dtype=BF16):
    ss = sum(jnp.sum(v * v, axis=-1, keepdims=True) for v in chunks)
    inv = lax.rsqrt(ss * (1.0 / D) + NORM_EPS)
    return [(v * inv * gain[:, i * NC:(i + 1) * NC]).astype(dtype) for i, v in enumerate(chunks)]


def body(hid_h, lens_h, ga_h, gf_h, gl_h, kv, wq, wo, wg, wu, wd, wh, H, S, G, DN,
         hid, lens, ga, gf, gl, in_sem, KV, X, Qf, Qs, O16, A, PS, CS, R1, R2,
         s_sem, g_sem, d_sem, kv_sem, q_ss, q_rs, o_ss, o_rs, ad_ss, ad_rs, al_ss, al_rs, af_ss, af_rs,
         p_ss, p_rs, c_ss, c_rs, h_ss, h_rs, x_sem):
    me = lax.axis_index('dp')
    c = lax.rem(me, 2)
    chip = me // 2
    partner = me + 1 - 2 * c
    other = lax.rem(me + 2, 4)
    my_row = pl.multiple_of(me * ROWS, ROWS)
    pa_row = pl.multiple_of(partner * ROWS, ROWS)
    chip_row = pl.multiple_of(chip * CHIP, CHIP)
    oth_row = pl.multiple_of((1 - chip) * CHIP, CHIP)

    def rdma(src, dst, ss, rs, dev):
        return pltpu.make_async_remote_copy(src_ref=src, dst_ref=dst, send_sem=ss, recv_sem=rs,
                                            device_id={'dp': dev}, device_id_type=MESH)

    def cp_wq(l, i):
        p, kk = i // 2, i % 2
        col = pl.multiple_of(c * QH + p * PAIR, 128)
        return pltpu.make_async_copy(wq.at[l, pl.ds(kk * 1024, 1024), pl.ds(col, PAIR)], S.at[i], s_sem.at[i])

    def cp_wo(l, i):
        col = pl.multiple_of(c * 1024, 128)
        return pltpu.make_async_copy(wo.at[l, pl.ds(i * 1024, 1024), pl.ds(col, 1024)],
                                     S.at[i, :, pl.ds(0, 1024)], s_sem.at[i])

    def cp_g(l, i):
        w, j = i % 2, i // 2
        src = wg if w == 0 else wu
        rows = NC if j < 5 else FFN - 5 * NC
        return pltpu.make_async_copy(src.at[l, pl.ds(j * NC, rows), :], G.at[w, pl.ds(j * NC, rows), :], g_sem.at[i])

    def dn_col(i):
        owner = 1 - c if i % 2 == 0 else c
        return 2 * owner + i // 2

    def cp_d(l, i):
        col = pl.multiple_of(dn_col(i) * NC, NC)
        return pltpu.make_async_copy(wd.at[l, :, pl.ds(col, NC)], DN.at[i, pl.ds(0, FFN), :], d_sem.at[i])

    def cp_kv(l, i):
        return pltpu.make_async_copy(kv.at[l, pl.ds(i * 8, 8)], KV.at[pl.ds(i * 8, 8)], kv_sem.at[i])

    def cp_hs(i):
        return pltpu.make_async_copy(wh.at[pl.ds((i % 2) * 1024, 1024), pl.ds((i // 2) * 1024, 1024)],
                                     S.at[i, :, pl.ds(0, 1024)], s_sem.at[i])

    def cp_hg(i):
        g, j = i // 4, i % 4
        return pltpu.make_async_copy(wh.at[pl.ds(j * 512, 512), pl.ds(4096 + g * D, D)],
                                     G.at[g, pl.ds(j * 512, 512), :], g_sem.at[i])

    def cp_hd(i):
        return pltpu.make_async_copy(wh.at[:, pl.ds(8192 + i * NC, NC)], DN.at[i, pl.ds(0, D), :], d_sem.at[i])

    def cp_hx(i):
        if i >= 4:
            g = i - 4
            return pltpu.make_async_copy(wh.at[pl.ds(g * 640, 640), pl.ds(10240, D)],
                                         G.at[g, pl.ds(D, 640), :], x_sem.at[i])
        return pltpu.make_async_copy(wh.at[pl.ds(1280, 768), pl.ds(10240 + i * NC, NC)],
                                     DN.at[i, pl.ds(D, 768), :], x_sem.at[i])

    ins = [pltpu.make_async_copy(a, b, in_sem.at[i]) for i, (a, b) in enumerate(
        ((hid_h, hid), (lens_h, lens), (ga_h, ga), (gf_h, gf), (gl_h, gl)))]
    for cp in ins:
        cp.start()
    for i in range(4):
        cp_wq(0, i).start()

    bar = pltpu.get_barrier_semaphore()
    for dev in (partner, other):
        pl.semaphore_signal(bar, inc=1, device_id={'dp': dev}, device_id_type=MESH)
    pl.semaphore_wait(bar, 2)

    ins[0].wait()
    for n in range(4):
        X[n, pl.ds(my_row, ROWS), :] = hid[:, n * NC:(n + 1) * NC]
    hx = rdma(X.at[:, pl.ds(my_row, ROWS), :], X.at[:, pl.ds(my_row, ROWS), :], h_ss.at[0], h_rs.at[0], partner)
    hx.start()
    for i in range(4):
        DN[i, FFN:FFN_PAD, :] = jnp.zeros((FFN_PAD - FFN, NC), BF16)
    A[:, FFN_PAD - 128:FFN_PAD] = jnp.zeros((ALL, 128), BF16)
    for cp in ins[1:]:
        cp.wait()
    hx.wait_send()
    rdma(X.at[:, pl.ds(pa_row, ROWS), :], X.at[:, pl.ds(pa_row, ROWS), :], h_ss.at[0], h_rs.at[0], partner).wait_recv()

    def x_chunks(row, rows):
        return [X[n, pl.ds(row, rows), :].astype(F32) for n in range(4)]

    def norm_to_h(row, rows, h_row, gain):
        for n, v in enumerate(_rows_norm(x_chunks(row, rows), gain)):
            H[pl.ds(h_row, rows), n * NC:(n + 1) * NC] = v

    def own_n(j):
        return 2 * c + j

    def par_n(j):
        return 2 * (1 - c) + j

    def ad(j, n):
        r = X.at[n, pl.ds(chip_row, CHIP), :]
        return rdma(r, r, ad_ss.at[j], ad_rs.at[j], partner)

    def al(j, row):
        r = X.at[own_n(j), pl.ds(row, CHIP), :]
        return rdma(r, r, al_ss.at[j], al_rs.at[j], other)

    def af(j, n):
        r = X.at[n, pl.ds(oth_row, CHIP), :]
        return rdma(r, r, af_ss.at[j], af_rs.at[j], partner)

    def gather_start(j):
        al(j, chip_row).start()
        ad(j, own_n(j)).start()

    def gather_finish(*work):
        for j in range(2):
            if work:
                work[j]()
            al(j, oth_row).wait_recv()
            af(j, own_n(j)).start()
        if work:
            work[2]()
        for j in range(2):
            ad(j, par_n(j)).wait_recv()
        for j in range(2):
            af(j, par_n(j)).wait_recv()
        for j in range(2):
            al(j, chip_row).wait_send()
            ad(j, own_n(j)).wait_send()
            af(j, own_n(j)).wait_send()

    for l in range(LAYERS):
        norm_to_h(my_row, ROWS, 0, ga[l:l + 1, :])
        norm_to_h(pa_row, ROWS, ROWS, ga[l:l + 1, :])

        def q_send(p):
            dst = Qf.at[:, pl.ds(pl.multiple_of((c * 8 + 2 * p) * ROWS, ROWS), 2 * ROWS), :]
            return rdma(Qs.at[:, pl.ds(2 * p * ROWS, 2 * ROWS), :], dst, q_ss.at[p], q_rs.at[p], partner)

        def q_recv(p):
            dst = Qf.at[:, pl.ds(pl.multiple_of(((1 - c) * 8 + 2 * p) * ROWS, ROWS), 2 * ROWS), :]
            return rdma(dst, dst, q_ss.at[p], q_rs.at[p], partner)

        for p in range(4):
            cp_wq(l, 2 * p).wait()
            cp_wq(l, 2 * p + 1).wait()
            if l == 0:
                if p < 2:
                    cp_wq(0, 2 * p + 4).start()
                    cp_wq(0, 2 * p + 5).start()
                if p == 1:
                    for i in range(4):
                        cp_kv(0, i).start()
                if p == 2:
                    for i in range(4):
                        cp_wo(0, i).start()
            r = jnp.dot(H[0:CHIP, 0:1024], S[2 * p], preferred_element_type=F32)
            r = r + jnp.dot(H[0:CHIP, 1024:2048], S[2 * p + 1], preferred_element_type=F32)
            if l > 0 or p > 1:
                cp_wo(l, 2 * p).start()
                cp_wo(l, 2 * p + 1).start()
            r = r.astype(BF16).astype(F32)
            for j in range(2):
                rj = r[:, j * KV_W:(j + 1) * KV_W]
                row = pl.multiple_of((c * 8 + 2 * p + j) * ROWS, ROWS)
                rj = jnp.concatenate([rj, jnp.zeros((CHIP, 64), F32)], axis=1)
                for t in range(5):
                    v = rj[:, t * 128:(t + 1) * 128]
                    Qf[t, pl.ds(row, ROWS), :] = v[0:ROWS]
                    Qs[t, (2 * p + j) * ROWS:(2 * p + j + 1) * ROWS, :] = v[ROWS:CHIP]
            q_send(p).start()
        for p in range(4):
            q_recv(p).wait_recv()
        for p in range(4):
            q_send(p).wait_send()

        def o_send(g2):
            r0 = g2 * 16
            return rdma(O16.at[:, pl.ds(r0, 16), :], O16.at[:, pl.ds(ROWS + r0, 16), :],
                        o_ss.at[g2], o_rs.at[g2], partner)

        for g in range(4):
            cp_kv(l, g).wait()
            if l == 0 and g > 0:
                for i in range(4):
                    cp_g(0, 4 * (g - 1) + i).start()
            sc = []
            for i in range(8):
                b = g * 8 + i
                qb = jnp.concatenate([Qf[t, pl.ds(b, HEADS, stride=ROWS), :] for t in range(5)], axis=1)
                s = jnp.dot(qb[:, 0:KV_W].astype(BF16), KV[b], preferred_element_type=F32) * QK_SCALE
                pos = lax.broadcasted_iota(jnp.int32, (HEADS, SEQ), 1)
                sc.append(jnp.where(pos < lens[b], s, -1e30))
            s = jnp.concatenate(sc, axis=0)
            e = jnp.exp(s - jnp.max(s, axis=-1, keepdims=True))
            pr = (e / jnp.sum(e, axis=-1, keepdims=True)).astype(BF16)
            for i in range(8):
                b = g * 8 + i
                o = lax.dot_general(pr[i * HEADS:(i + 1) * HEADS], KV[b, 0:LATENT, :], (((1,), (1,)), ((), ())),
                                    preferred_element_type=F32)
                for t in range(4):
                    Qf[t, pl.ds(b, HEADS, stride=ROWS), :] = o[:, t * 128:(t + 1) * 128]
            if g % 2 == 1:
                r0 = (g // 2) * 16
                for h in range(HEADS):
                    for t in range(4):
                        O16[h, r0:r0 + 16, t * 128:(t + 1) * 128] = (
                            Qf[t, h * ROWS + r0:h * ROWS + r0 + 16, :].astype(BF16))
                o_send(g // 2).start()
        for g2 in range(2):
            r0 = g2 * 16
            ref = O16.at[:, pl.ds(ROWS + r0, 16), :]
            rdma(ref, ref, o_ss.at[g2], o_rs.at[g2], partner).wait_recv()
        for g2 in range(2):
            o_send(g2).wait_send()

        for i in range(8):
            cp_wo(l, i).wait()
        if l == 0:
            for i in range(4):
                cp_d(0, i).start()
        for j in range(2):
            acc = None
            for k in range(8):
                for hh in range(2):
                    t = jnp.dot(O16[2 * k + hh], S[k, hh * LATENT:(hh + 1) * LATENT, j * NC:(j + 1) * NC],
                                preferred_element_type=F32)
                    acc = t if acc is None else acc + t
            n = own_n(j)
            X[n, pl.ds(my_row, ROWS), :] = (X[n, pl.ds(my_row, ROWS), :].astype(F32) + acc[0:ROWS]).astype(BF16)
            X[n, pl.ds(pa_row, ROWS), :] = (X[n, pl.ds(pa_row, ROWS), :].astype(F32) + acc[ROWS:CHIP]).astype(BF16)
            gather_start(j)
        if l + 1 == LAYERS:
            for i in range(8):
                cp_hs(i).start()

        def flip(k):
            w, j = k % 2, k // 2
            cp_g(l, k).wait()

            def step(i, carry):
                row = pl.multiple_of(j * NC + i * 256, 256)
                for q in range(8):
                    G[w, pl.ds(row, 256), q * 256:(q + 1) * 256] = G[w, pl.ds(row, 256), q * 256:(q + 1) * 256].T
                return carry

            lax.fori_loop(0, 2, step, 0)

        def flips(a, b):
            def work():
                for k in range(a, b):
                    flip(k)
            return work

        gather_finish(flips(0, 7), flips(7, 9), flips(9, 10))

        for r in range(4):
            norm_to_h(r * ROWS, ROWS, r * ROWS, gf[l:l + 1, :])
        if l + 1 < LAYERS:
            for i in range(8):
                cp_wq(l + 1, i).start()
            for i in range(4):
                cp_kv(l + 1, i).start()
        for i in range(10, 12):
            cp_g(l, i).wait()

        def ffn_cols(n0, size):
            g_ = lax.dot_general(H[...], G[0, pl.ds(n0, size), :], (((1,), (1,)), ((), ())),
                                 preferred_element_type=F32)
            u_ = lax.dot_general(H[...], G[1, pl.ds(n0, size), :], (((1,), (1,)), ((), ())),
                                 preferred_element_type=F32)
            A[:, pl.ds(n0, size)] = (jax.nn.silu(g_) * u_).astype(BF16)

        def ffn_step(n, carry):
            for half in range(2):
                row = pl.multiple_of(n * NC + half * 256, 256)
                gu = []
                for w in range(2):
                    acc = None
                    for q in range(8):
                        t = jnp.dot(H[:, q * 256:(q + 1) * 256], G[w, pl.ds(row, 256), q * 256:(q + 1) * 256],
                                    preferred_element_type=F32)
                        acc = t if acc is None else acc + t
                    gu.append(acc)
                A[:, pl.ds(row, 256)] = (jax.nn.silu(gu[0]) * gu[1]).astype(BF16)
            return carry

        lax.fori_loop(0, 5, ffn_step, 0)
        ffn_cols(5 * NC, FFN - 5 * NC)
        if l + 1 < LAYERS:
            for i in range(12):
                cp_g(l + 1, i).start()
        else:
            for i in range(8):
                cp_hg(i).start()
            for i in range(4, 6):
                cp_hx(i).start()

        def ps(j):
            return rdma(PS.at[j], R1.at[j], p_ss.at[j], p_rs.at[j], partner)

        def cs(j):
            return rdma(CS.at[j, pl.ds(oth_row, CHIP), :], R2.at[j], c_ss.at[j], c_rs.at[j], other)

        def down(i):
            cp_d(l, i).wait()
            y = jnp.dot(A[...], DN[i], preferred_element_type=F32)
            if l + 1 < LAYERS:
                cp_d(l + 1, i).start()
            else:
                cp_hd(i).start()
                cp_hx(i).start()
            return y

        def chip_sum(j):
            ps(j).wait_recv()
            CS[j] = CS[j] + R1[j]
            cs(j).start()

        PS[0] = down(0)
        ps(0).start()
        CS[0] = down(1)
        PS[1] = down(2)
        ps(1).start()
        chip_sum(0)
        CS[1] = down(3)
        chip_sum(1)
        last = l + 1 == LAYERS
        for j in range(2):
            cs(j).wait_recv()
            n = own_n(j)
            xr = X[n, pl.ds(chip_row, CHIP), :].astype(F32)
            X[n, pl.ds(chip_row, CHIP), :] = (xr + (CS[j, pl.ds(chip_row, CHIP), :] + R2[j])).astype(BF16)
            if last:
                gather_start(j)
            else:
                ad(j, own_n(j)).start()
        for j in range(2):
            ps(j).wait_send()
            cs(j).wait_send()
        if last:
            gather_finish()
        else:
            for j in range(2):
                ad(j, par_n(j)).wait_recv()
            for j in range(2):
                ad(j, own_n(j)).wait_send()

    for r in range(4):
        norm_to_h(r * ROWS, ROWS, r * ROWS, gl[...])
    for i in range(8):
        cp_hs(i).wait()
        cp_hg(i).wait()
    for i in range(4):
        cp_hd(i).wait()
        cp_hx(i).wait()
    for i in range(4, 6):
        cp_hx(i).wait()


RING = 4
BLOCKS = VOCAB // NC
HELD = 24
STREAM = BLOCKS - HELD


def head_body(H, S, G, DN, wh, out, W, OH, OS, w_sem, oh_sem, os_sem):
    def cp_w(t, slot):
        col = pl.multiple_of((HELD + t) * NC, NC)
        return pltpu.make_async_copy(wh.at[:, pl.ds(col, NC)], W.at[slot], w_sem.at[slot])

    def cp_out(buf, sems, block, slot):
        col = pl.multiple_of(block * NC, NC)
        return pltpu.make_async_copy(buf.at[slot], out.at[:, pl.ds(col, NC)], sems.at[slot])

    for t in range(RING):
        cp_w(t, t).start()

    def stream(t):
        slot, o = lax.rem(t, RING), lax.rem(t, 2)
        cp_w(t, slot).wait()

        @pl.when(t >= 2)
        def _():
            cp_out(OS, os_sem, HELD + t, o).wait()

        OS[o] = jnp.dot(H[...], W[slot], preferred_element_type=F32)
        cp_out(OS, os_sem, HELD + t, o).start()

        @pl.when(t + RING < STREAM)
        def _():
            cp_w(t + RING, slot).start()

    def held(t, value):
        o = lax.rem(t, 2)

        @pl.when(t >= 2)
        def _():
            cp_out(OH, oh_sem, t, o).wait()

        OH[o] = value()
        cp_out(OH, oh_sem, t, o).start()

    def dot(a, b):
        return jnp.dot(a, b, preferred_element_type=F32)

    def seg_s(t, carry):
        p, col = t // 2, pl.multiple_of(lax.rem(t, 2) * NC, NC)
        held(t, lambda: dot(H[:, 0:1024], S[2 * p, :, pl.ds(col, NC)])
             + dot(H[:, 1024:2048], S[2 * p + 1, :, pl.ds(col, NC)]))
        stream(t)
        return carry

    def seg_g(t, carry):
        g, col = t // 4 - 2, pl.multiple_of(lax.rem(t, 4) * NC, NC)
        held(t, lambda: dot(H[...], G[g, 0:D, pl.ds(col, NC)]))
        stream(t)
        return carry

    def seg_d(t, carry):
        held(t, lambda: dot(H[...], DN[t - 16, 0:D, :]))
        stream(t)
        return carry

    def seg_x(t, carry):
        col = pl.multiple_of((t - 20) * NC, NC)
        held(t, lambda: dot(H[:, 0:640], G[0, D:D + 640, pl.ds(col, NC)])
             + dot(H[:, 640:1280], G[1, D:D + 640, pl.ds(col, NC)])
             + dot(H[:, 1280:2048], DN[t - 20, D:D + 768, :]))
        stream(t)
        return carry

    def seg_w(t, carry):
        stream(t)
        return carry

    lax.fori_loop(0, 8, seg_s, 0)
    lax.fori_loop(8, 16, seg_g, 0)
    lax.fori_loop(16, 20, seg_d, 0)
    lax.fori_loop(20, 24, seg_x, 0)
    lax.fori_loop(24, STREAM, seg_w, 0)
    for o in range(2):
        cp_out(OH, oh_sem, HELD - 2 + o, o).wait()
        cp_out(OS, os_sem, BLOCKS - 2 + o, o).wait()


def head_kernel(normed, s_buf, g_buf, d_buf, w_head):
    vm = pl.BlockSpec(memory_space=pltpu.VMEM)
    hb = pl.BlockSpec(memory_space=pl.ANY)
    dma = pltpu.SemaphoreType.DMA
    held = [pltpu.with_memory_space_constraint(a, pltpu.VMEM) for a in (normed, s_buf, g_buf, d_buf)]
    return pl.pallas_call(
        head_body,
        out_shape=jax.ShapeDtypeStruct((ALL, VOCAB), F32),
        in_specs=[vm] * 4 + [hb],
        out_specs=hb,
        scratch_shapes=[pltpu.VMEM((RING, D, NC), BF16), pltpu.VMEM((2, ALL, NC), F32), pltpu.VMEM((2, ALL, NC), F32),
                        dma((RING,)), dma((2,)), dma((2,))],
        compiler_params=pltpu.CompilerParams(vmem_limit_bytes=13500000),
        name='head',
    )(*held, w_head)


def layers_kernel(hidden, lengths, kv_t, norm_attn, w_q, w_o, norm_ffn, wg_t, wu_t, w_down, norm_final, w_head):
    hb = pl.BlockSpec(memory_space=pl.ANY)
    dma = pltpu.SemaphoreType.DMA
    vm = pl.BlockSpec(memory_space=pltpu.VMEM)
    scratch = [
        pltpu.VMEM((ROWS, D), BF16), pltpu.SMEM((ROWS,), jnp.int32), pltpu.VMEM((2, D), F32), pltpu.VMEM((2, D), F32),
        pltpu.VMEM((1, D), F32), dma((5,)),
        pltpu.VMEM((ROWS, KV_W, SEQ), BF16),
        pltpu.VMEM((4, ALL, NC), BF16),
        pltpu.VMEM((5, HEADS * ROWS, 128), F32),
        pltpu.VMEM((5, 8 * ROWS, 128), F32),
        pltpu.VMEM((HEADS, CHIP, LATENT), BF16),
        pltpu.VMEM((ALL, FFN_PAD), BF16),
        pltpu.VMEM((2, ALL, NC), F32),
        pltpu.VMEM((2, ALL, NC), F32),
        pltpu.VMEM((2, ALL, NC), F32),
        pltpu.VMEM((2, CHIP, NC), F32),
        dma((8,)), dma((12,)), dma((4,)), dma((4,)),
        dma((4,)), dma((4,)), dma((2,)), dma((2,)),
        dma((2,)), dma((2,)), dma((2,)), dma((2,)), dma((2,)), dma((2,)),
        dma((2,)), dma((2,)), dma((2,)), dma((2,)), dma((1,)), dma((1,)), dma((6,)),
    ]
    return pl.pallas_call(
        body,
        out_shape=[pltpu.VMEM((ALL, D), BF16), pltpu.VMEM((8, 1024, PAIR), BF16), pltpu.VMEM((2, FFN, D), BF16),
                   pltpu.VMEM((4, FFN_PAD, NC), BF16)],
        in_specs=[hb] * 12,
        out_specs=[vm] * 4,
        scratch_shapes=scratch,
        compiler_params=pltpu.CompilerParams(collective_id=0, has_side_effects=True, vmem_limit_bytes=13500000),
        name='layers',
    )(hidden, lengths, norm_attn, norm_ffn, norm_final.reshape(1, D), kv_t, w_q, w_o, wg_t, wu_t, w_down, w_head)


def solution(mesh):
    row_axes = ('rep', 'dp')
    specs_in = (P(row_axes, None), P(row_axes), P(None, row_axes, None, None), P(), P(), P(), P(),
                P(None, None, 'dp'), P(None, None, 'dp'), P(None, 'dp', None), P(), P(None, 'dp'))

    def device_step(hidden, lengths, kv_cache, norm_attn, w_q, w_o, norm_ffn, w_gate, w_up, w_down, norm_final, w_head):
        held = layers_kernel(hidden, lengths, jnp.swapaxes(kv_cache, 2, 3), norm_attn, w_q, w_o, norm_ffn,
                               jnp.swapaxes(w_gate, 1, 2), jnp.swapaxes(w_up, 1, 2), w_down, norm_final, w_head)
        return head_kernel(*held, w_head)

    return jax.shard_map(device_step, mesh=mesh, in_specs=specs_in, out_specs=P('rep', 'dp'), check_vma=False)
```

```python
import functools

import jax
import jax.numpy as jnp
from jax import lax
from jax.experimental import pallas as pl
from jax.experimental.pallas import tpu as pltpu
from jax.sharding import PartitionSpec as P

F32 = jnp.float32
BF16 = jnp.bfloat16
MESH = pl.DeviceIdType.MESH

D = 2048
HEADS = 16
LATENT = 512
KV_W = 576
SEQ = 128
ROWS = 32
CHIP = 64
ALL = 128
FFN = 2736
FFN_PAD = 2816
NC = 512
QH = HEADS * KV_W // 2
PAIR = 2 * KV_W
VOCAB = 25600
QK_SCALE = 192 ** -0.5
NORM_EPS = 1e-6
LAYERS = 2


def _rows_norm(chunks, gain, dtype=BF16):
    ss = sum(jnp.sum(v * v, axis=-1, keepdims=True) for v in chunks)
    inv = lax.rsqrt(ss * (1.0 / D) + NORM_EPS)
    return [(v * inv * gain[:, i * NC:(i + 1) * NC]).astype(dtype) for i, v in enumerate(chunks)]


def body(hid_h, lens_h, ga_h, gf_h, gl_h, kv, wq, wo, wg, wu, wd, wh, H, S, G, DN,
         hid, lens, ga, gf, gl, in_sem, KV, X, Qf, Qs, O16, A, PS, CS, R1, R2,
         s_sem, g_sem, d_sem, kv_sem, q_ss, q_rs, o_ss, o_rs, ad_ss, ad_rs, al_ss, al_rs, af_ss, af_rs,
         p_ss, p_rs, c_ss, c_rs, h_ss, h_rs, x_sem):
    me = lax.axis_index('dp')
    c = lax.rem(me, 2)
    chip = me // 2
    partner = me + 1 - 2 * c
    other = lax.rem(me + 2, 4)
    my_row = pl.multiple_of(me * ROWS, ROWS)
    pa_row = pl.multiple_of(partner * ROWS, ROWS)
    chip_row = pl.multiple_of(chip * CHIP, CHIP)
    oth_row = pl.multiple_of((1 - chip) * CHIP, CHIP)

    def rdma(src, dst, ss, rs, dev):
        return pltpu.make_async_remote_copy(src_ref=src, dst_ref=dst, send_sem=ss, recv_sem=rs,
                                            device_id={'dp': dev}, device_id_type=MESH)

    def cp_wq(l, i):
        p, kk = i // 2, i % 2
        col = pl.multiple_of(c * QH + p * PAIR, 128)
        return pltpu.make_async_copy(wq.at[l, pl.ds(kk * 1024, 1024), pl.ds(col, PAIR)], S.at[i], s_sem.at[i])

    def cp_wo(l, i):
        col = pl.multiple_of(c * 1024, 128)
        return pltpu.make_async_copy(wo.at[l, pl.ds(i * 1024, 1024), pl.ds(col, 1024)],
                                     S.at[i, :, pl.ds(0, 1024)], s_sem.at[i])

    def cp_g(l, i):
        w, j = i % 2, i // 2
        src = wg if w == 0 else wu
        rows = NC if j < 5 else FFN - 5 * NC
        return pltpu.make_async_copy(src.at[l, pl.ds(j * NC, rows), :], G.at[w, pl.ds(j * NC, rows), :], g_sem.at[i])

    def dn_col(i):
        owner = 1 - c if i % 2 == 0 else c
        return 2 * owner + i // 2

    def cp_d(l, i):
        col = pl.multiple_of(dn_col(i) * NC, NC)
        return pltpu.make_async_copy(wd.at[l, :, pl.ds(col, NC)], DN.at[i, pl.ds(0, FFN), :], d_sem.at[i])

    def cp_kv(l, i):
        return pltpu.make_async_copy(kv.at[l, pl.ds(i * 8, 8)], KV.at[pl.ds(i * 8, 8)], kv_sem.at[i])

    def cp_hs(i):
        return pltpu.make_async_copy(wh.at[pl.ds((i % 2) * 1024, 1024), pl.ds((i // 2) * 1024, 1024)],
                                     S.at[i, :, pl.ds(0, 1024)], s_sem.at[i])

    def cp_hg(i):
        g, j = i // 4, i % 4
        return pltpu.make_async_copy(wh.at[pl.ds(j * 512, 512), pl.ds(4096 + g * D, D)],
                                     G.at[g, pl.ds(j * 512, 512), :], g_sem.at[i])

    def cp_hd(i):
        return pltpu.make_async_copy(wh.at[:, pl.ds(8192 + i * NC, NC)], DN.at[i, pl.ds(0, D), :], d_sem.at[i])

    def cp_hx(i):
        if i >= 4:
            g = i - 4
            return pltpu.make_async_copy(wh.at[pl.ds(g * 640, 640), pl.ds(10240, D)],
                                         G.at[g, pl.ds(D, 640), :], x_sem.at[i])
        return pltpu.make_async_copy(wh.at[pl.ds(1280, 768), pl.ds(10240 + i * NC, NC)],
                                     DN.at[i, pl.ds(D, 768), :], x_sem.at[i])

    ins = [pltpu.make_async_copy(a, b, in_sem.at[i]) for i, (a, b) in enumerate(
        ((hid_h, hid), (lens_h, lens), (ga_h, ga), (gf_h, gf), (gl_h, gl)))]
    for cp in ins:
        cp.start()
    for i in range(4):
        cp_wq(0, i).start()

    bar = pltpu.get_barrier_semaphore()
    for dev in (partner, other):
        pl.semaphore_signal(bar, inc=1, device_id={'dp': dev}, device_id_type=MESH)
    pl.semaphore_wait(bar, 2)

    ins[0].wait()
    for n in range(4):
        X[n, pl.ds(my_row, ROWS), :] = hid[:, n * NC:(n + 1) * NC]
    hx = rdma(X.at[:, pl.ds(my_row, ROWS), :], X.at[:, pl.ds(my_row, ROWS), :], h_ss.at[0], h_rs.at[0], partner)
    hx.start()
    for i in range(4):
        DN[i, FFN:FFN_PAD, :] = jnp.zeros((FFN_PAD - FFN, NC), BF16)
    A[:, FFN_PAD - 128:FFN_PAD] = jnp.zeros((ALL, 128), BF16)
    for cp in ins[1:]:
        cp.wait()
    hx.wait_send()
    rdma(X.at[:, pl.ds(pa_row, ROWS), :], X.at[:, pl.ds(pa_row, ROWS), :], h_ss.at[0], h_rs.at[0], partner).wait_recv()

    def x_chunks(row, rows):
        return [X[n, pl.ds(row, rows), :].astype(F32) for n in range(4)]

    def norm_to_h(row, rows, h_row, gain):
        for n, v in enumerate(_rows_norm(x_chunks(row, rows), gain)):
            H[pl.ds(h_row, rows), n * NC:(n + 1) * NC] = v

    def own_n(j):
        return 2 * c + j

    def par_n(j):
        return 2 * (1 - c) + j

    def ad(j, n):
        r = X.at[n, pl.ds(chip_row, CHIP), :]
        return rdma(r, r, ad_ss.at[j], ad_rs.at[j], partner)

    def al(j, row):
        r = X.at[own_n(j), pl.ds(row, CHIP), :]
        return rdma(r, r, al_ss.at[j], al_rs.at[j], other)

    def af(j, n):
        r = X.at[n, pl.ds(oth_row, CHIP), :]
        return rdma(r, r, af_ss.at[j], af_rs.at[j], partner)

    def gather_start(j):
        al(j, chip_row).start()
        ad(j, own_n(j)).start()

    def gather_finish(*work):
        for j in range(2):
            if work:
                work[j]()
            al(j, oth_row).wait_recv()
            af(j, own_n(j)).start()
        if work:
            work[2]()
        for j in range(2):
            ad(j, par_n(j)).wait_recv()
        for j in range(2):
            af(j, par_n(j)).wait_recv()
        for j in range(2):
            al(j, chip_row).wait_send()
            ad(j, own_n(j)).wait_send()
            af(j, own_n(j)).wait_send()

    for l in range(LAYERS):
        norm_to_h(my_row, ROWS, 0, ga[l:l + 1, :])
        norm_to_h(pa_row, ROWS, ROWS, ga[l:l + 1, :])

        def q_send(p):
            dst = Qf.at[:, pl.ds(pl.multiple_of((c * 8 + 2 * p) * ROWS, ROWS), 2 * ROWS), :]
            return rdma(Qs.at[:, pl.ds(2 * p * ROWS, 2 * ROWS), :], dst, q_ss.at[p], q_rs.at[p], partner)

        def q_recv(p):
            dst = Qf.at[:, pl.ds(pl.multiple_of(((1 - c) * 8 + 2 * p) * ROWS, ROWS), 2 * ROWS), :]
            return rdma(dst, dst, q_ss.at[p], q_rs.at[p], partner)

        for p in range(4):
            cp_wq(l, 2 * p).wait()
            cp_wq(l, 2 * p + 1).wait()
            if l == 0:
                if p < 2:
                    cp_wq(0, 2 * p + 4).start()
                    cp_wq(0, 2 * p + 5).start()
            r = jnp.dot(H[0:CHIP, 0:1024], S[2 * p], preferred_element_type=F32)
            r = r + jnp.dot(H[0:CHIP, 1024:2048], S[2 * p + 1], preferred_element_type=F32)
            r = r.astype(BF16).astype(F32)
            for j in range(2):
                rj = r[:, j * KV_W:(j + 1) * KV_W]
                row = pl.multiple_of((c * 8 + 2 * p + j) * ROWS, ROWS)
                rj = jnp.concatenate([rj, jnp.zeros((CHIP, 64), F32)], axis=1)
                for t in range(5):
                    v = rj[:, t * 128:(t + 1) * 128]
                    Qf[t, pl.ds(row, ROWS), :] = v[0:ROWS]
                    Qs[t, (2 * p + j) * ROWS:(2 * p + j + 1) * ROWS, :] = v[ROWS:CHIP]
            q_send(p).start()
            if l == 0 and p == 1:
                for i in range(4):
                    cp_kv(0, i).start()
        for i in range(8):
            cp_wo(l, i).start()
        for p in range(4):
            q_recv(p).wait_recv()
        for p in range(4):
            q_send(p).wait_send()

        def o_send(g2):
            r0 = g2 * 16
            return rdma(O16.at[:, pl.ds(r0, 16), :], O16.at[:, pl.ds(ROWS + r0, 16), :],
                        o_ss.at[g2], o_rs.at[g2], partner)

        for g in range(4):
            cp_kv(l, g).wait()
            sc = []
            for i in range(8):
                b = g * 8 + i
                qb = jnp.concatenate([Qf[t, pl.ds(b, HEADS, stride=ROWS), :] for t in range(5)], axis=1)
                s = jnp.dot(qb[:, 0:KV_W].astype(BF16), KV[b], preferred_element_type=F32) * QK_SCALE
                pos = lax.broadcasted_iota(jnp.int32, (HEADS, SEQ), 1)
                sc.append(jnp.where(pos < lens[b], s, -1e30))
            s = jnp.concatenate(sc, axis=0)
            e = jnp.exp(s - jnp.max(s, axis=-1, keepdims=True))
            pr = (e / jnp.sum(e, axis=-1, keepdims=True)).astype(BF16)
            for i in range(8):
                b = g * 8 + i
                o = lax.dot_general(pr[i * HEADS:(i + 1) * HEADS], KV[b, 0:LATENT, :], (((1,), (1,)), ((), ())),
                                    preferred_element_type=F32)
                for t in range(4):
                    Qf[t, pl.ds(b, HEADS, stride=ROWS), :] = o[:, t * 128:(t + 1) * 128]
            if g % 2 == 1:
                r0 = (g // 2) * 16
                for h in range(HEADS):
                    for t in range(4):
                        O16[h, r0:r0 + 16, t * 128:(t + 1) * 128] = (
                            Qf[t, h * ROWS + r0:h * ROWS + r0 + 16, :].astype(BF16))
                o_send(g // 2).start()
        if l == 0:
            for i in range(4):
                cp_g(0, i).start()
        else:
            for i in range(4):
                cp_d(l, i).start()
        for g2 in range(2):
            r0 = g2 * 16
            ref = O16.at[:, pl.ds(ROWS + r0, 16), :]
            rdma(ref, ref, o_ss.at[g2], o_rs.at[g2], partner).wait_recv()
        for g2 in range(2):
            o_send(g2).wait_send()

        for i in range(8):
            cp_wo(l, i).wait()
        for j in range(2):
            acc = None
            for k in range(8):
                for hh in range(2):
                    t = jnp.dot(O16[2 * k + hh], S[k, hh * LATENT:(hh + 1) * LATENT, j * NC:(j + 1) * NC],
                                preferred_element_type=F32)
                    acc = t if acc is None else acc + t
            n = own_n(j)
            X[n, pl.ds(my_row, ROWS), :] = (X[n, pl.ds(my_row, ROWS), :].astype(F32) + acc[0:ROWS]).astype(BF16)
            X[n, pl.ds(pa_row, ROWS), :] = (X[n, pl.ds(pa_row, ROWS), :].astype(F32) + acc[ROWS:CHIP]).astype(BF16)
            gather_start(j)
        if l == 0:
            for i in range(4, 12):
                cp_g(0, i).start()

        def flip(k):
            w, j = k % 2, k // 2
            cp_g(l, k).wait()

            def step(i, carry):
                row = pl.multiple_of(j * NC + i * 256, 256)
                for q in range(8):
                    G[w, pl.ds(row, 256), q * 256:(q + 1) * 256] = G[w, pl.ds(row, 256), q * 256:(q + 1) * 256].T
                return carry

            lax.fori_loop(0, 2, step, 0)

        def flips(a, b):
            def work():
                for k in range(a, b):
                    flip(k)
            return work

        def rest():
            if l == 0:
                for i in range(4):
                    cp_d(0, i).start()
            flip(9)

        gather_finish(flips(0, 7), flips(7, 9), rest)

        for r in range(4):
            norm_to_h(r * ROWS, ROWS, r * ROWS, gf[l:l + 1, :])
        if l + 1 < LAYERS:
            for i in range(4):
                cp_wq(l + 1, i).start()
        else:
            for i in range(6):
                cp_hs(i).start()
        for i in range(10, 12):
            cp_g(l, i).wait()

        def ffn_cols(n0, size):
            g_ = lax.dot_general(H[...], G[0, pl.ds(n0, size), :], (((1,), (1,)), ((), ())),
                                 preferred_element_type=F32)
            u_ = lax.dot_general(H[...], G[1, pl.ds(n0, size), :], (((1,), (1,)), ((), ())),
                                 preferred_element_type=F32)
            A[:, pl.ds(n0, size)] = (jax.nn.silu(g_) * u_).astype(BF16)

        def ffn_step(n, carry):
            for half in range(2):
                row = pl.multiple_of(n * NC + half * 256, 256)
                gu = []
                for w in range(2):
                    acc = None
                    for q in range(8):
                        t = jnp.dot(H[:, q * 256:(q + 1) * 256], G[w, pl.ds(row, 256), q * 256:(q + 1) * 256],
                                    preferred_element_type=F32)
                        acc = t if acc is None else acc + t
                    gu.append(acc)
                A[:, pl.ds(row, 256)] = (jax.nn.silu(gu[0]) * gu[1]).astype(BF16)
            return carry

        lax.fori_loop(0, 5, ffn_step, 0)
        ffn_cols(5 * NC, FFN - 5 * NC)

        def ps(j):
            return rdma(PS.at[j], R1.at[j], p_ss.at[j], p_rs.at[j], partner)

        def cs(j):
            return rdma(CS.at[j, pl.ds(oth_row, CHIP), :], R2.at[j], c_ss.at[j], c_rs.at[j], other)

        def down(i):
            cp_d(l, i).wait()
            return jnp.dot(A[...], DN[i], preferred_element_type=F32)

        def chip_sum(j):
            ps(j).wait_recv()
            CS[j] = CS[j] + R1[j]
            cs(j).start()

        PS[0] = down(0)
        ps(0).start()
        CS[0] = down(1)
        PS[1] = down(2)
        ps(1).start()
        chip_sum(0)
        CS[1] = down(3)
        chip_sum(1)
        last = l + 1 == LAYERS
        if last:
            for i in range(6, 8):
                cp_hs(i).start()
            for i in range(8):
                cp_hg(i).start()
            for i in range(4, 6):
                cp_hx(i).start()
        else:
            for i in range(4, 8):
                cp_wq(l + 1, i).start()
            for i in range(4):
                cp_kv(l + 1, i).start()
            for i in range(8):
                cp_g(l + 1, i).start()
        for j in range(2):
            cs(j).wait_recv()
            n = own_n(j)
            xr = X[n, pl.ds(chip_row, CHIP), :].astype(F32)
            X[n, pl.ds(chip_row, CHIP), :] = (xr + (CS[j, pl.ds(chip_row, CHIP), :] + R2[j])).astype(BF16)
            if last:
                gather_start(j)
            else:
                ad(j, own_n(j)).start()
        if last:
            for i in range(4):
                cp_hd(i).start()
                cp_hx(i).start()
        else:
            for i in range(8, 12):
                cp_g(l + 1, i).start()
        for j in range(2):
            ps(j).wait_send()
            cs(j).wait_send()
        if last:
            gather_finish()
        else:
            for j in range(2):
                ad(j, par_n(j)).wait_recv()
            for j in range(2):
                ad(j, own_n(j)).wait_send()

    for r in range(4):
        norm_to_h(r * ROWS, ROWS, r * ROWS, gl[...])
    for i in range(8):
        cp_hs(i).wait()
        cp_hg(i).wait()
    for i in range(4):
        cp_hd(i).wait()
        cp_hx(i).wait()
    for i in range(4, 6):
        cp_hx(i).wait()


RING = 4
BLOCKS = VOCAB // NC
HELD = 24
STREAM = BLOCKS - HELD


def head_body(H, S, G, DN, wh, out, W, OH, OS, w_sem, oh_sem, os_sem):
    def cp_w(t, slot):
        col = pl.multiple_of((HELD + t) * NC, NC)
        return pltpu.make_async_copy(wh.at[:, pl.ds(col, NC)], W.at[slot], w_sem.at[slot])

    def cp_out(buf, sems, block, slot):
        col = pl.multiple_of(block * NC, NC)
        return pltpu.make_async_copy(buf.at[slot], out.at[:, pl.ds(col, NC)], sems.at[slot])

    for t in range(RING):
        cp_w(t, t).start()

    def stream(t):
        slot, o = lax.rem(t, RING), lax.rem(t, 2)
        cp_w(t, slot).wait()

        @pl.when(t >= 2)
        def _():
            cp_out(OS, os_sem, HELD + t, o).wait()

        OS[o] = jnp.dot(H[...], W[slot], preferred_element_type=F32)
        cp_out(OS, os_sem, HELD + t, o).start()

        @pl.when(t + RING < STREAM)
        def _():
            cp_w(t + RING, slot).start()

    def held(t, value):
        o = lax.rem(t, 2)

        @pl.when(t >= 2)
        def _():
            cp_out(OH, oh_sem, t, o).wait()

        OH[o] = value()
        cp_out(OH, oh_sem, t, o).start()

    def dot(a, b):
        return jnp.dot(a, b, preferred_element_type=F32)

    def seg_s(t, carry):
        p, col = t // 2, pl.multiple_of(lax.rem(t, 2) * NC, NC)
        held(t, lambda: dot(H[:, 0:1024], S[2 * p, :, pl.ds(col, NC)])
             + dot(H[:, 1024:2048], S[2 * p + 1, :, pl.ds(col, NC)]))
        stream(t)
        return carry

    def seg_g(t, carry):
        g, col = t // 4 - 2, pl.multiple_of(lax.rem(t, 4) * NC, NC)
        held(t, lambda: dot(H[...], G[g, 0:D, pl.ds(col, NC)]))
        stream(t)
        return carry

    def seg_d(t, carry):
        held(t, lambda: dot(H[...], DN[t - 16, 0:D, :]))
        stream(t)
        return carry

    def seg_x(t, carry):
        col = pl.multiple_of((t - 20) * NC, NC)
        held(t, lambda: dot(H[:, 0:640], G[0, D:D + 640, pl.ds(col, NC)])
             + dot(H[:, 640:1280], G[1, D:D + 640, pl.ds(col, NC)])
             + dot(H[:, 1280:2048], DN[t - 20, D:D + 768, :]))
        stream(t)
        return carry

    def seg_w(t, carry):
        stream(t)
        return carry

    lax.fori_loop(0, 8, seg_s, 0)
    lax.fori_loop(8, 16, seg_g, 0)
    lax.fori_loop(16, 20, seg_d, 0)
    lax.fori_loop(20, 24, seg_x, 0)
    lax.fori_loop(24, STREAM, seg_w, 0)
    for o in range(2):
        cp_out(OH, oh_sem, HELD - 2 + o, o).wait()
        cp_out(OS, os_sem, BLOCKS - 2 + o, o).wait()


def head_kernel(normed, s_buf, g_buf, d_buf, w_head):
    vm = pl.BlockSpec(memory_space=pltpu.VMEM)
    hb = pl.BlockSpec(memory_space=pl.ANY)
    dma = pltpu.SemaphoreType.DMA
    held = [pltpu.with_memory_space_constraint(a, pltpu.VMEM) for a in (normed, s_buf, g_buf, d_buf)]
    return pl.pallas_call(
        head_body,
        out_shape=jax.ShapeDtypeStruct((ALL, VOCAB), F32),
        in_specs=[vm] * 4 + [hb],
        out_specs=hb,
        scratch_shapes=[pltpu.VMEM((RING, D, NC), BF16), pltpu.VMEM((2, ALL, NC), F32), pltpu.VMEM((2, ALL, NC), F32),
                        dma((RING,)), dma((2,)), dma((2,))],
        compiler_params=pltpu.CompilerParams(vmem_limit_bytes=13500000),
        name='head',
    )(*held, w_head)


def layers_kernel(hidden, lengths, kv_t, norm_attn, w_q, w_o, norm_ffn, wg_t, wu_t, w_down, norm_final, w_head):
    hb = pl.BlockSpec(memory_space=pl.ANY)
    dma = pltpu.SemaphoreType.DMA
    vm = pl.BlockSpec(memory_space=pltpu.VMEM)
    scratch = [
        pltpu.VMEM((ROWS, D), BF16), pltpu.SMEM((ROWS,), jnp.int32), pltpu.VMEM((2, D), F32), pltpu.VMEM((2, D), F32),
        pltpu.VMEM((1, D), F32), dma((5,)),
        pltpu.VMEM((ROWS, KV_W, SEQ), BF16),
        pltpu.VMEM((4, ALL, NC), BF16),
        pltpu.VMEM((5, HEADS * ROWS, 128), F32),
        pltpu.VMEM((5, 8 * ROWS, 128), F32),
        pltpu.VMEM((HEADS, CHIP, LATENT), BF16),
        pltpu.VMEM((ALL, FFN_PAD), BF16),
        pltpu.VMEM((2, ALL, NC), F32),
        pltpu.VMEM((2, ALL, NC), F32),
        pltpu.VMEM((2, ALL, NC), F32),
        pltpu.VMEM((2, CHIP, NC), F32),
        dma((8,)), dma((12,)), dma((4,)), dma((4,)),
        dma((4,)), dma((4,)), dma((2,)), dma((2,)),
        dma((2,)), dma((2,)), dma((2,)), dma((2,)), dma((2,)), dma((2,)),
        dma((2,)), dma((2,)), dma((2,)), dma((2,)), dma((1,)), dma((1,)), dma((6,)),
    ]
    return pl.pallas_call(
        body,
        out_shape=[pltpu.VMEM((ALL, D), BF16), pltpu.VMEM((8, 1024, PAIR), BF16), pltpu.VMEM((2, FFN, D), BF16),
                   pltpu.VMEM((4, FFN_PAD, NC), BF16)],
        in_specs=[hb] * 12,
        out_specs=[vm] * 4,
        scratch_shapes=scratch,
        compiler_params=pltpu.CompilerParams(collective_id=0, has_side_effects=True, vmem_limit_bytes=13500000),
        name='layers',
    )(hidden, lengths, norm_attn, norm_ffn, norm_final.reshape(1, D), kv_t, w_q, w_o, wg_t, wu_t, w_down, w_head)


def solution(mesh):
    row_axes = ('rep', 'dp')
    specs_in = (P(row_axes, None), P(row_axes), P(None, row_axes, None, None), P(), P(), P(), P(),
                P(None, None, 'dp'), P(None, None, 'dp'), P(None, 'dp', None), P(), P(None, 'dp'))

    def device_step(hidden, lengths, kv_cache, norm_attn, w_q, w_o, norm_ffn, w_gate, w_up, w_down, norm_final, w_head):
        held = layers_kernel(hidden, lengths, jnp.swapaxes(kv_cache, 2, 3), norm_attn, w_q, w_o, norm_ffn,
                               jnp.swapaxes(w_gate, 1, 2), jnp.swapaxes(w_up, 1, 2), w_down, norm_final, w_head)
        return head_kernel(*held, w_head)

    return jax.shard_map(device_step, mesh=mesh, in_specs=specs_in, out_specs=P('rep', 'dp'), check_vma=False)
```

```python
import functools

import jax
import jax.numpy as jnp
from jax import lax
from jax.experimental import pallas as pl
from jax.experimental.pallas import tpu as pltpu
from jax.sharding import PartitionSpec as P

F32 = jnp.float32
BF16 = jnp.bfloat16
MESH = pl.DeviceIdType.MESH

D = 2048
HEADS = 16
LATENT = 512
KV_W = 576
SEQ = 128
ROWS = 32
CHIP = 64
ALL = 128
FFN = 2736
FFN_PAD = 2816
NC = 512
XC = 256
XN = D // XC
U = XN // 2
QH = HEADS * KV_W // 2
PAIR = 2 * KV_W
VOCAB = 25600
QK_SCALE = 192 ** -0.5
NORM_EPS = 1e-6
LAYERS = 2


def _rows_norm(chunks, gain, dtype=BF16):
    ss = sum(jnp.sum(v * v, axis=-1, keepdims=True) for v in chunks)
    inv = lax.rsqrt(ss * (1.0 / D) + NORM_EPS)
    return [(v * inv * gain[:, i * XC:(i + 1) * XC]).astype(dtype) for i, v in enumerate(chunks)]


def body(hid_h, lens_h, ga_h, gf_h, gl_h, kv, wq, wo, wg, wu, wd, wh, H, S, G, DN,
         hid, lens, ga, gf, gl, in_sem, KV, X, Qf, Qs, O16, A, PS, CS, R1, R2,
         s_sem, g_sem, d_sem, kv_sem, q_ss, q_rs, o_ss, o_rs, ad_ss, ad_rs, al_ss, al_rs, af_ss, af_rs,
         p_ss, p_rs, c_ss, c_rs, h_ss, h_rs, x_sem):
    me = lax.axis_index('dp')
    c = lax.rem(me, 2)
    chip = me // 2
    partner = me + 1 - 2 * c
    other = lax.rem(me + 2, 4)
    my_row = pl.multiple_of(me * ROWS, ROWS)
    pa_row = pl.multiple_of(partner * ROWS, ROWS)
    chip_row = pl.multiple_of(chip * CHIP, CHIP)
    oth_row = pl.multiple_of((1 - chip) * CHIP, CHIP)

    def rdma(src, dst, ss, rs, dev):
        return pltpu.make_async_remote_copy(src_ref=src, dst_ref=dst, send_sem=ss, recv_sem=rs,
                                            device_id={'dp': dev}, device_id_type=MESH)

    def cp_wq(l, i):
        p, kk = i // 2, i % 2
        col = pl.multiple_of(c * QH + p * PAIR, 128)
        return pltpu.make_async_copy(wq.at[l, pl.ds(kk * 1024, 1024), pl.ds(col, PAIR)], S.at[i], s_sem.at[i])

    def cp_wo(l, i):
        col = pl.multiple_of(c * 1024, 128)
        return pltpu.make_async_copy(wo.at[l, pl.ds(i * 1024, 1024), pl.ds(col, 1024)],
                                     S.at[i, :, pl.ds(0, 1024)], s_sem.at[i])

    def cp_g(l, i):
        w, j = i % 2, i // 2
        src = wg if w == 0 else wu
        rows = NC if j < 5 else FFN - 5 * NC
        return pltpu.make_async_copy(src.at[l, pl.ds(j * NC, rows), :], G.at[w, pl.ds(j * NC, rows), :], g_sem.at[i])

    def dn_col(i):
        owner = 1 - c if i % 2 == 0 else c
        return 2 * owner + i // 2

    def cp_d(l, i):
        col = pl.multiple_of(dn_col(i) * NC, NC)
        return pltpu.make_async_copy(wd.at[l, :, pl.ds(col, NC)], DN.at[i, pl.ds(0, FFN), :], d_sem.at[i])

    def cp_kv(l, i):
        return pltpu.make_async_copy(kv.at[l, pl.ds(i * 8, 8)], KV.at[pl.ds(i * 8, 8)], kv_sem.at[i])

    def cp_hs(i):
        return pltpu.make_async_copy(wh.at[pl.ds((i % 2) * 1024, 1024), pl.ds((i // 2) * 1024, 1024)],
                                     S.at[i, :, pl.ds(0, 1024)], s_sem.at[i])

    def cp_hg(i):
        g, j = i // 4, i % 4
        return pltpu.make_async_copy(wh.at[pl.ds(j * 512, 512), pl.ds(4096 + g * D, D)],
                                     G.at[g, pl.ds(j * 512, 512), :], g_sem.at[i])

    def cp_hd(i):
        return pltpu.make_async_copy(wh.at[:, pl.ds(8192 + i * NC, NC)], DN.at[i, pl.ds(0, D), :], d_sem.at[i])

    def cp_hx(i):
        if i >= 4:
            g = i - 4
            return pltpu.make_async_copy(wh.at[pl.ds(g * 640, 640), pl.ds(10240, D)],
                                         G.at[g, pl.ds(D, 640), :], x_sem.at[i])
        return pltpu.make_async_copy(wh.at[pl.ds(1280, 768), pl.ds(10240 + i * NC, NC)],
                                     DN.at[i, pl.ds(D, 768), :], x_sem.at[i])

    ins = [pltpu.make_async_copy(a, b, in_sem.at[i]) for i, (a, b) in enumerate(
        ((hid_h, hid), (lens_h, lens), (ga_h, ga), (gf_h, gf), (gl_h, gl)))]
    for cp in ins:
        cp.start()
    for i in range(4):
        cp_wq(0, i).start()

    bar = pltpu.get_barrier_semaphore()
    for dev in (partner, other):
        pl.semaphore_signal(bar, inc=1, device_id={'dp': dev}, device_id_type=MESH)
    pl.semaphore_wait(bar, 2)

    ins[0].wait()
    for n in range(XN):
        X[n, pl.ds(my_row, ROWS), :] = hid[:, n * XC:(n + 1) * XC]
    hx = rdma(X.at[:, pl.ds(my_row, ROWS), :], X.at[:, pl.ds(my_row, ROWS), :], h_ss.at[0], h_rs.at[0], partner)
    hx.start()
    for i in range(4):
        DN[i, FFN:FFN_PAD, :] = jnp.zeros((FFN_PAD - FFN, NC), BF16)
    A[:, FFN_PAD - 128:FFN_PAD] = jnp.zeros((ALL, 128), BF16)
    for cp in ins[1:]:
        cp.wait()
    hx.wait_send()
    rdma(X.at[:, pl.ds(pa_row, ROWS), :], X.at[:, pl.ds(pa_row, ROWS), :], h_ss.at[0], h_rs.at[0], partner).wait_recv()

    def x_chunks(row, rows):
        return [X[n, pl.ds(row, rows), :].astype(F32) for n in range(XN)]

    def norm_to_h(row, rows, h_row, gain):
        for n, v in enumerate(_rows_norm(x_chunks(row, rows), gain)):
            H[pl.ds(h_row, rows), n * XC:(n + 1) * XC] = v

    def own_n(j):
        return U * c + j

    def par_n(j):
        return U * (1 - c) + j

    def ad(j, n):
        r = X.at[n, pl.ds(chip_row, CHIP), :]
        return rdma(r, r, ad_ss.at[j], ad_rs.at[j], partner)

    def al(j, row):
        r = X.at[own_n(j), pl.ds(row, CHIP), :]
        return rdma(r, r, al_ss.at[j], al_rs.at[j], other)

    def af(j, n):
        r = X.at[n, pl.ds(oth_row, CHIP), :]
        return rdma(r, r, af_ss.at[j], af_rs.at[j], partner)

    def gather_start(j):
        al(j, chip_row).start()
        ad(j, own_n(j)).start()

    def gather_finish(*work):
        for j in range(U):
            if work:
                work[j]()
            al(j, oth_row).wait_recv()
            af(j, own_n(j)).start()
        for w in work[U:]:
            w()
        for j in range(U):
            ad(j, par_n(j)).wait_recv()
        for j in range(U):
            af(j, par_n(j)).wait_recv()
        for j in range(U):
            al(j, chip_row).wait_send()
            ad(j, own_n(j)).wait_send()
            af(j, own_n(j)).wait_send()

    for l in range(LAYERS):
        norm_to_h(my_row, ROWS, 0, ga[l:l + 1, :])
        norm_to_h(pa_row, ROWS, ROWS, ga[l:l + 1, :])

        def q_send(p):
            dst = Qf.at[:, pl.ds(pl.multiple_of((c * 8 + 2 * p) * ROWS, ROWS), 2 * ROWS), :]
            return rdma(Qs.at[:, pl.ds(2 * p * ROWS, 2 * ROWS), :], dst, q_ss.at[p], q_rs.at[p], partner)

        def q_recv(p):
            dst = Qf.at[:, pl.ds(pl.multiple_of(((1 - c) * 8 + 2 * p) * ROWS, ROWS), 2 * ROWS), :]
            return rdma(dst, dst, q_ss.at[p], q_rs.at[p], partner)

        for p in range(4):
            cp_wq(l, 2 * p).wait()
            cp_wq(l, 2 * p + 1).wait()
            if l == 0:
                if p < 2:
                    cp_wq(0, 2 * p + 4).start()
                    cp_wq(0, 2 * p + 5).start()
                if p == 1:
                    for i in range(4):
                        cp_kv(0, i).start()
                if p == 2:
                    for i in range(4):
                        cp_wo(0, i).start()
            r = jnp.dot(H[0:CHIP, 0:1024], S[2 * p], preferred_element_type=F32)
            r = r + jnp.dot(H[0:CHIP, 1024:2048], S[2 * p + 1], preferred_element_type=F32)
            if l > 0 or p > 1:
                cp_wo(l, 2 * p).start()
                cp_wo(l, 2 * p + 1).start()
            r = r.astype(BF16).astype(F32)
            for j in range(2):
                rj = r[:, j * KV_W:(j + 1) * KV_W]
                row = pl.multiple_of((c * 8 + 2 * p + j) * ROWS, ROWS)
                rj = jnp.concatenate([rj, jnp.zeros((CHIP, 64), F32)], axis=1)
                for t in range(5):
                    v = rj[:, t * 128:(t + 1) * 128]
                    Qf[t, pl.ds(row, ROWS), :] = v[0:ROWS]
                    Qs[t, (2 * p + j) * ROWS:(2 * p + j + 1) * ROWS, :] = v[ROWS:CHIP]
            q_send(p).start()
        for p in range(4):
            q_recv(p).wait_recv()
        for p in range(4):
            q_send(p).wait_send()

        def o_send(g2):
            r0 = g2 * 16
            return rdma(O16.at[:, pl.ds(r0, 16), :], O16.at[:, pl.ds(ROWS + r0, 16), :],
                        o_ss.at[g2], o_rs.at[g2], partner)

        for g in range(4):
            cp_kv(l, g).wait()
            if l == 0 and g > 0:
                for i in range(4):
                    cp_g(0, 4 * (g - 1) + i).start()
            sc = []
            for i in range(8):
                b = g * 8 + i
                qb = jnp.concatenate([Qf[t, pl.ds(b, HEADS, stride=ROWS), :] for t in range(5)], axis=1)
                s = jnp.dot(qb[:, 0:KV_W].astype(BF16), KV[b], preferred_element_type=F32) * QK_SCALE
                pos = lax.broadcasted_iota(jnp.int32, (HEADS, SEQ), 1)
                sc.append(jnp.where(pos < lens[b], s, -1e30))
            s = jnp.concatenate(sc, axis=0)
            e = jnp.exp(s - jnp.max(s, axis=-1, keepdims=True))
            pr = (e / jnp.sum(e, axis=-1, keepdims=True)).astype(BF16)
            for i in range(8):
                b = g * 8 + i
                o = lax.dot_general(pr[i * HEADS:(i + 1) * HEADS], KV[b, 0:LATENT, :], (((1,), (1,)), ((), ())),
                                    preferred_element_type=F32)
                for t in range(4):
                    Qf[t, pl.ds(b, HEADS, stride=ROWS), :] = o[:, t * 128:(t + 1) * 128]
            if g % 2 == 1:
                r0 = (g // 2) * 16
                for h in range(HEADS):
                    for t in range(4):
                        O16[h, r0:r0 + 16, t * 128:(t + 1) * 128] = (
                            Qf[t, h * ROWS + r0:h * ROWS + r0 + 16, :].astype(BF16))
                o_send(g // 2).start()
        for g2 in range(2):
            r0 = g2 * 16
            ref = O16.at[:, pl.ds(ROWS + r0, 16), :]
            rdma(ref, ref, o_ss.at[g2], o_rs.at[g2], partner).wait_recv()
        for g2 in range(2):
            o_send(g2).wait_send()

        for i in range(8):
            cp_wo(l, i).wait()
        if l == 0:
            for i in range(4):
                cp_d(0, i).start()
        for j in range(U):
            acc = []
            for hh in range(2):
                a = None
                for k in range(8):
                    t = jnp.dot(O16[2 * k + hh], S[k, hh * LATENT:(hh + 1) * LATENT, j * XC:(j + 1) * XC],
                                preferred_element_type=F32)
                    a = t if a is None else a + t
                acc.append(a)
            acc = acc[0] + acc[1]
            n = own_n(j)
            X[n, pl.ds(my_row, ROWS), :] = (X[n, pl.ds(my_row, ROWS), :].astype(F32) + acc[0:ROWS]).astype(BF16)
            X[n, pl.ds(pa_row, ROWS), :] = (X[n, pl.ds(pa_row, ROWS), :].astype(F32) + acc[ROWS:CHIP]).astype(BF16)
            gather_start(j)
        if l + 1 == LAYERS:
            for i in range(8):
                cp_hs(i).start()

        def flip(k):
            w, j = k % 2, k // 2
            cp_g(l, k).wait()

            for row in range(j * NC, (j + 1) * NC, 256):
                for q in range(8):
                    G[w, row:row + 256, q * 256:(q + 1) * 256] = G[w, row:row + 256, q * 256:(q + 1) * 256].T

        def flips(a, b):
            def work():
                for k in range(a, b):
                    flip(k)
            return work

        gather_finish(flips(0, 4), flips(4, 6), flips(6, 8), flips(8, 9), flips(9, 10))

        for r in range(4):
            norm_to_h(r * ROWS, ROWS, r * ROWS, gf[l:l + 1, :])
        if l + 1 < LAYERS:
            for i in range(8):
                cp_wq(l + 1, i).start()
            for i in range(4):
                cp_kv(l + 1, i).start()
        for i in range(10, 12):
            cp_g(l, i).wait()

        def ffn_cols(n0, size):
            g_ = lax.dot_general(H[...], G[0, pl.ds(n0, size), :], (((1,), (1,)), ((), ())),
                                 preferred_element_type=F32)
            u_ = lax.dot_general(H[...], G[1, pl.ds(n0, size), :], (((1,), (1,)), ((), ())),
                                 preferred_element_type=F32)
            A[:, pl.ds(n0, size)] = (jax.nn.silu(g_) * u_).astype(BF16)

        def ffn_step(n, carry):
            for half in range(2):
                row = pl.multiple_of(n * NC + half * 256, 256)
                gu = []
                for w in range(2):
                    acc = None
                    for q in range(8):
                        t = jnp.dot(H[:, q * 256:(q + 1) * 256], G[w, pl.ds(row, 256), q * 256:(q + 1) * 256],
                                    preferred_element_type=F32)
                        acc = t if acc is None else acc + t
                    gu.append(acc)
                A[:, pl.ds(row, 256)] = (jax.nn.silu(gu[0]) * gu[1]).astype(BF16)
            return carry

        lax.fori_loop(0, 5, ffn_step, 0)
        ffn_cols(5 * NC, FFN - 5 * NC)
        if l + 1 < LAYERS:
            for i in range(12):
                cp_g(l + 1, i).start()
        else:
            for i in range(8):
                cp_hg(i).start()
            for i in range(4, 6):
                cp_hx(i).start()

        def ps(j):
            return rdma(PS.at[j], R1.at[j], p_ss.at[j], p_rs.at[j], partner)

        def cs(j):
            return rdma(CS.at[j, pl.ds(oth_row, CHIP), :], R2.at[j], c_ss.at[j], c_rs.at[j], other)

        def down(i, half, buf):
            k = 6 * 256
            col = half * XC
            buf[i // 2 * 2 + half] = (
                jnp.dot(A[:, 0:k], DN[i, 0:k, col:col + XC], preferred_element_type=F32)
                + jnp.dot(A[:, k:FFN_PAD], DN[i, k:FFN_PAD, col:col + XC], preferred_element_type=F32))

        def next_d(i):
            if l + 1 < LAYERS:
                cp_d(l + 1, i).start()
            else:
                cp_hd(i).start()
                cp_hx(i).start()

        def chip_sum(j):
            ps(j).wait_recv()
            CS[j] = CS[j] + R1[j]
            cs(j).start()

        for i in range(4):
            cp_d(l, i).wait()
            for half in range(2):
                if i % 2 == 0:
                    down(i, half, PS)
                    ps(i + half).start()
                else:
                    down(i, half, CS)
            next_d(i)
            if i >= 2:
                for j in (2 * i - 4, 2 * i - 3):
                    chip_sum(j)
        last = l + 1 == LAYERS
        for j in range(U):
            cs(j).wait_recv()
            n = own_n(j)
            xr = X[n, pl.ds(chip_row, CHIP), :].astype(F32)
            X[n, pl.ds(chip_row, CHIP), :] = (xr + (CS[j, pl.ds(chip_row, CHIP), :] + R2[j])).astype(BF16)
            if last:
                gather_start(j)
            else:
                ad(j, own_n(j)).start()
        for j in range(U):
            ps(j).wait_send()
            cs(j).wait_send()
        if last:
            gather_finish()
        else:
            for j in range(U):
                ad(j, par_n(j)).wait_recv()
            for j in range(U):
                ad(j, own_n(j)).wait_send()

    for r in range(4):
        norm_to_h(r * ROWS, ROWS, r * ROWS, gl[...])
    for i in range(8):
        cp_hs(i).wait()
        cp_hg(i).wait()
    for i in range(4):
        cp_hd(i).wait()
        cp_hx(i).wait()
    for i in range(4, 6):
        cp_hx(i).wait()


RING = 4
BLOCKS = VOCAB // NC
HELD = 24
STREAM = BLOCKS - HELD


def head_body(H, S, G, DN, wh, out, W, OH, OS, w_sem, oh_sem, os_sem):
    def cp_w(t, slot):
        col = pl.multiple_of((HELD + t) * NC, NC)
        return pltpu.make_async_copy(wh.at[:, pl.ds(col, NC)], W.at[slot], w_sem.at[slot])

    def cp_out(buf, sems, block, slot):
        col = pl.multiple_of(block * NC, NC)
        return pltpu.make_async_copy(buf.at[slot], out.at[:, pl.ds(col, NC)], sems.at[slot])

    for t in range(RING):
        cp_w(t, t).start()

    def stream(t):
        slot, o = lax.rem(t, RING), lax.rem(t, 2)
        cp_w(t, slot).wait()

        @pl.when(t >= 2)
        def _():
            cp_out(OS, os_sem, HELD + t, o).wait()

        OS[o] = jnp.dot(H[...], W[slot], preferred_element_type=F32)
        cp_out(OS, os_sem, HELD + t, o).start()

        @pl.when(t + RING < STREAM)
        def _():
            cp_w(t + RING, slot).start()

    def held(t, value):
        o = lax.rem(t, 2)

        @pl.when(t >= 2)
        def _():
            cp_out(OH, oh_sem, t, o).wait()

        OH[o] = value()
        cp_out(OH, oh_sem, t, o).start()

    def dot(a, b):
        return jnp.dot(a, b, preferred_element_type=F32)

    def seg_s(t, carry):
        p, col = t // 2, pl.multiple_of(lax.rem(t, 2) * NC, NC)
        held(t, lambda: dot(H[:, 0:1024], S[2 * p, :, pl.ds(col, NC)])
             + dot(H[:, 1024:2048], S[2 * p + 1, :, pl.ds(col, NC)]))
        stream(t)
        return carry

    def seg_g(t, carry):
        g, col = t // 4 - 2, pl.multiple_of(lax.rem(t, 4) * NC, NC)
        held(t, lambda: dot(H[...], G[g, 0:D, pl.ds(col, NC)]))
        stream(t)
        return carry

    def seg_d(t, carry):
        held(t, lambda: dot(H[...], DN[t - 16, 0:D, :]))
        stream(t)
        return carry

    def seg_x(t, carry):
        col = pl.multiple_of((t - 20) * NC, NC)
        held(t, lambda: dot(H[:, 0:640], G[0, D:D + 640, pl.ds(col, NC)])
             + dot(H[:, 640:1280], G[1, D:D + 640, pl.ds(col, NC)])
             + dot(H[:, 1280:2048], DN[t - 20, D:D + 768, :]))
        stream(t)
        return carry

    def seg_w(t, carry):
        stream(t)
        return carry

    lax.fori_loop(0, 8, seg_s, 0)
    lax.fori_loop(8, 16, seg_g, 0)
    lax.fori_loop(16, 20, seg_d, 0)
    lax.fori_loop(20, 24, seg_x, 0)
    lax.fori_loop(24, STREAM, seg_w, 0)
    for o in range(2):
        cp_out(OH, oh_sem, HELD - 2 + o, o).wait()
        cp_out(OS, os_sem, BLOCKS - 2 + o, o).wait()


def head_kernel(normed, s_buf, g_buf, d_buf, w_head):
    vm = pl.BlockSpec(memory_space=pltpu.VMEM)
    hb = pl.BlockSpec(memory_space=pl.ANY)
    dma = pltpu.SemaphoreType.DMA
    held = [pltpu.with_memory_space_constraint(a, pltpu.VMEM) for a in (normed, s_buf, g_buf, d_buf)]
    return pl.pallas_call(
        head_body,
        out_shape=jax.ShapeDtypeStruct((ALL, VOCAB), F32),
        in_specs=[vm] * 4 + [hb],
        out_specs=hb,
        scratch_shapes=[pltpu.VMEM((RING, D, NC), BF16), pltpu.VMEM((2, ALL, NC), F32), pltpu.VMEM((2, ALL, NC), F32),
                        dma((RING,)), dma((2,)), dma((2,))],
        compiler_params=pltpu.CompilerParams(vmem_limit_bytes=13500000),
        name='head',
    )(*held, w_head)


def layers_kernel(hidden, lengths, kv_t, norm_attn, w_q, w_o, norm_ffn, wg_t, wu_t, w_down, norm_final, w_head):
    hb = pl.BlockSpec(memory_space=pl.ANY)
    dma = pltpu.SemaphoreType.DMA
    vm = pl.BlockSpec(memory_space=pltpu.VMEM)
    scratch = [
        pltpu.VMEM((ROWS, D), BF16), pltpu.SMEM((ROWS,), jnp.int32), pltpu.VMEM((2, D), F32), pltpu.VMEM((2, D), F32),
        pltpu.VMEM((1, D), F32), dma((5,)),
        pltpu.VMEM((ROWS, KV_W, SEQ), BF16),
        pltpu.VMEM((XN, ALL, XC), BF16),
        pltpu.VMEM((5, HEADS * ROWS, 128), F32),
        pltpu.VMEM((5, 8 * ROWS, 128), F32),
        pltpu.VMEM((HEADS, CHIP, LATENT), BF16),
        pltpu.VMEM((ALL, FFN_PAD), BF16),
        pltpu.VMEM((U, ALL, XC), F32),
        pltpu.VMEM((U, ALL, XC), F32),
        pltpu.VMEM((U, ALL, XC), F32),
        pltpu.VMEM((U, CHIP, XC), F32),
        dma((8,)), dma((12,)), dma((4,)), dma((4,)),
        dma((4,)), dma((4,)), dma((2,)), dma((2,)),
        dma((U,)), dma((U,)), dma((U,)), dma((U,)), dma((U,)), dma((U,)),
        dma((U,)), dma((U,)), dma((U,)), dma((U,)), dma((1,)), dma((1,)), dma((6,)),
    ]
    return pl.pallas_call(
        body,
        out_shape=[pltpu.VMEM((ALL, D), BF16), pltpu.VMEM((8, 1024, PAIR), BF16), pltpu.VMEM((2, FFN, D), BF16),
                   pltpu.VMEM((4, FFN_PAD, NC), BF16)],
        in_specs=[hb] * 12,
        out_specs=[vm] * 4,
        scratch_shapes=scratch,
        compiler_params=pltpu.CompilerParams(collective_id=0, has_side_effects=True, vmem_limit_bytes=13500000),
        name='layers',
    )(hidden, lengths, norm_attn, norm_ffn, norm_final.reshape(1, D), kv_t, w_q, w_o, wg_t, wu_t, w_down, w_head)


def solution(mesh):
    row_axes = ('rep', 'dp')
    specs_in = (P(row_axes, None), P(row_axes), P(None, row_axes, None, None), P(), P(), P(), P(),
                P(None, None, 'dp'), P(None, None, 'dp'), P(None, 'dp', None), P(), P(None, 'dp'))

    def device_step(hidden, lengths, kv_cache, norm_attn, w_q, w_o, norm_ffn, w_gate, w_up, w_down, norm_final, w_head):
        held = layers_kernel(hidden, lengths, jnp.swapaxes(kv_cache, 2, 3), norm_attn, w_q, w_o, norm_ffn,
                               jnp.swapaxes(w_gate, 1, 2), jnp.swapaxes(w_up, 1, 2), w_down, norm_final, w_head)
        return head_kernel(*held, w_head)

    return jax.shard_map(device_step, mesh=mesh, in_specs=specs_in, out_specs=P('rep', 'dp'), check_vma=False)
```

```python
import functools

import jax
import jax.numpy as jnp
from jax import lax
from jax.experimental import pallas as pl
from jax.experimental.pallas import tpu as pltpu
from jax.sharding import PartitionSpec as P

F32 = jnp.float32
BF16 = jnp.bfloat16
MESH = pl.DeviceIdType.MESH

D = 2048
HEADS = 16
LATENT = 512
KV_W = 576
SEQ = 128
ROWS = 32
CHIP = 64
ALL = 128
FFN = 2736
FFN_PAD = 2816
NC = 512
QH = HEADS * KV_W // 2
PAIR = 2 * KV_W
VOCAB = 25600
QK_SCALE = 192 ** -0.5
NORM_EPS = 1e-6
LAYERS = 2


def _rows_norm(chunks, gain, dtype=BF16):
    ss = sum(jnp.sum(v * v, axis=-1, keepdims=True) for v in chunks)
    inv = lax.rsqrt(ss * (1.0 / D) + NORM_EPS)
    return [(v * inv * gain[:, i * NC:(i + 1) * NC]).astype(dtype) for i, v in enumerate(chunks)]


def body(hid_h, lens_h, ga_h, gf_h, gl_h, kv, wq, wo, wg, wu, wd, wh, H, S, G, DN,
         hid, lens, ga, gf, gl, in_sem, KV, X, Qf, Qs, O16, A, PS, CS, R1, R2,
         s_sem, g_sem, d_sem, kv_sem, q_ss, q_rs, o_ss, o_rs, ad_ss, ad_rs, al_ss, al_rs, af_ss, af_rs,
         p_ss, p_rs, c_ss, c_rs, h_ss, h_rs, x_sem):
    me = lax.axis_index('dp')
    c = lax.rem(me, 2)
    chip = me // 2
    partner = me + 1 - 2 * c
    other = lax.rem(me + 2, 4)
    my_row = pl.multiple_of(me * ROWS, ROWS)
    pa_row = pl.multiple_of(partner * ROWS, ROWS)
    chip_row = pl.multiple_of(chip * CHIP, CHIP)
    oth_row = pl.multiple_of((1 - chip) * CHIP, CHIP)

    def rdma(src, dst, ss, rs, dev):
        return pltpu.make_async_remote_copy(src_ref=src, dst_ref=dst, send_sem=ss, recv_sem=rs,
                                            device_id={'dp': dev}, device_id_type=MESH)

    def cp_wq(l, i):
        p, kk = i // 2, i % 2
        col = pl.multiple_of(c * QH + p * PAIR, 128)
        return pltpu.make_async_copy(wq.at[l, pl.ds(kk * 1024, 1024), pl.ds(col, PAIR)], S.at[i], s_sem.at[i])

    def cp_wo(l, i):
        col = pl.multiple_of(c * 1024, 128)
        return pltpu.make_async_copy(wo.at[l, pl.ds(i * 1024, 1024), pl.ds(col, 1024)],
                                     S.at[i, :, pl.ds(0, 1024)], s_sem.at[i])

    def cp_g(l, i):
        w, j = i % 2, i // 2
        src = wg if w == 0 else wu
        rows = NC if j < 5 else FFN - 5 * NC
        return pltpu.make_async_copy(src.at[l, pl.ds(j * NC, rows), :], G.at[w, pl.ds(j * NC, rows), :], g_sem.at[i])

    def dn_col(i):
        owner = 1 - c if i % 2 == 0 else c
        return 2 * owner + i // 2

    def cp_d(l, i):
        col = pl.multiple_of(dn_col(i) * NC, NC)
        return pltpu.make_async_copy(wd.at[l, :, pl.ds(col, NC)], DN.at[i, pl.ds(0, FFN), :], d_sem.at[i])

    def cp_kv(l, i):
        return pltpu.make_async_copy(kv.at[l, pl.ds(i * 8, 8)], KV.at[pl.ds(i * 8, 8)], kv_sem.at[i])

    def cp_hs(i):
        return pltpu.make_async_copy(wh.at[pl.ds((i % 2) * 1024, 1024), pl.ds((i // 2) * 1024, 1024)],
                                     S.at[i, :, pl.ds(0, 1024)], s_sem.at[i])

    def cp_hg(i):
        g, j = i // 4, i % 4
        return pltpu.make_async_copy(wh.at[pl.ds(j * 512, 512), pl.ds(4096 + g * D, D)],
                                     G.at[g, pl.ds(j * 512, 512), :], g_sem.at[i])

    def cp_hd(i):
        return pltpu.make_async_copy(wh.at[:, pl.ds(8192 + i * NC, NC)], DN.at[i, pl.ds(0, D), :], d_sem.at[i])

    def cp_hx(i):
        if i >= 4:
            g = i - 4
            return pltpu.make_async_copy(wh.at[pl.ds(g * 640, 640), pl.ds(10240, D)],
                                         G.at[g, pl.ds(D, 640), :], x_sem.at[i])
        return pltpu.make_async_copy(wh.at[pl.ds(1280, 768), pl.ds(10240 + i * NC, NC)],
                                     DN.at[i, pl.ds(D, 768), :], x_sem.at[i])

    ins = [pltpu.make_async_copy(a, b, in_sem.at[i]) for i, (a, b) in enumerate(
        ((hid_h, hid), (lens_h, lens), (ga_h, ga), (gf_h, gf), (gl_h, gl)))]
    for cp in ins:
        cp.start()
    for i in range(4):
        cp_wq(0, i).start()

    bar = pltpu.get_barrier_semaphore()
    for dev in (partner, other):
        pl.semaphore_signal(bar, inc=1, device_id={'dp': dev}, device_id_type=MESH)
    pl.semaphore_wait(bar, 2)

    ins[0].wait()
    for n in range(4):
        X[n, pl.ds(my_row, ROWS), :] = hid[:, n * NC:(n + 1) * NC]
    hx = rdma(X.at[:, pl.ds(my_row, ROWS), :], X.at[:, pl.ds(my_row, ROWS), :], h_ss.at[0], h_rs.at[0], partner)
    hx.start()
    for i in range(4):
        DN[i, FFN:FFN_PAD, :] = jnp.zeros((FFN_PAD - FFN, NC), BF16)
    A[:, FFN_PAD - 128:FFN_PAD] = jnp.zeros((ALL, 128), BF16)
    for cp in ins[1:]:
        cp.wait()
    hx.wait_send()
    rdma(X.at[:, pl.ds(pa_row, ROWS), :], X.at[:, pl.ds(pa_row, ROWS), :], h_ss.at[0], h_rs.at[0], partner).wait_recv()

    def x_chunks(row, rows):
        return [X[n, pl.ds(row, rows), :].astype(F32) for n in range(4)]

    def norm_to_h(row, rows, h_row, gain):
        for n, v in enumerate(_rows_norm(x_chunks(row, rows), gain)):
            H[pl.ds(h_row, rows), n * NC:(n + 1) * NC] = v

    def own_n(j):
        return 2 * c + j

    def par_n(j):
        return 2 * (1 - c) + j

    def ad(j, n):
        r = X.at[n, pl.ds(chip_row, CHIP), :]
        return rdma(r, r, ad_ss.at[j], ad_rs.at[j], partner)

    def al(j, row):
        r = X.at[own_n(j), pl.ds(row, CHIP), :]
        return rdma(r, r, al_ss.at[j], al_rs.at[j], other)

    def af(j, n):
        r = X.at[n, pl.ds(oth_row, CHIP), :]
        return rdma(r, r, af_ss.at[j], af_rs.at[j], partner)

    def gather_start(j):
        al(j, chip_row).start()
        ad(j, own_n(j)).start()

    def gather_finish(*work):
        for j in range(2):
            if work:
                work[j]()
            al(j, oth_row).wait_recv()
            af(j, own_n(j)).start()
        if work:
            work[2]()
        for j in range(2):
            ad(j, par_n(j)).wait_recv()
        for j in range(2):
            af(j, par_n(j)).wait_recv()
        for j in range(2):
            al(j, chip_row).wait_send()
            ad(j, own_n(j)).wait_send()
            af(j, own_n(j)).wait_send()

    for l in range(LAYERS):
        norm_to_h(my_row, ROWS, 0, ga[l:l + 1, :])
        norm_to_h(pa_row, ROWS, ROWS, ga[l:l + 1, :])

        def q_send(p):
            dst = Qf.at[:, pl.ds(pl.multiple_of((c * 8 + 2 * p) * ROWS, ROWS), 2 * ROWS), :]
            return rdma(Qs.at[:, pl.ds(2 * p * ROWS, 2 * ROWS), :], dst, q_ss.at[p], q_rs.at[p], partner)

        def q_recv(p):
            dst = Qf.at[:, pl.ds(pl.multiple_of(((1 - c) * 8 + 2 * p) * ROWS, ROWS), 2 * ROWS), :]
            return rdma(dst, dst, q_ss.at[p], q_rs.at[p], partner)

        for p in range(4):
            cp_wq(l, 2 * p).wait()
            cp_wq(l, 2 * p + 1).wait()
            if l == 0:
                if p < 2:
                    cp_wq(0, 2 * p + 4).start()
                    cp_wq(0, 2 * p + 5).start()
                if p == 1:
                    for i in range(4):
                        cp_kv(0, i).start()
                if p == 2:
                    for i in range(4):
                        cp_wo(0, i).start()
            r = jnp.dot(H[0:CHIP, 0:1024], S[2 * p], preferred_element_type=F32)
            r = r + jnp.dot(H[0:CHIP, 1024:2048], S[2 * p + 1], preferred_element_type=F32)
            if l > 0 or p > 1:
                cp_wo(l, 2 * p).start()
                cp_wo(l, 2 * p + 1).start()
            r = r.astype(BF16).astype(F32)
            for j in range(2):
                rj = r[:, j * KV_W:(j + 1) * KV_W]
                row = pl.multiple_of((c * 8 + 2 * p + j) * ROWS, ROWS)
                rj = jnp.concatenate([rj, jnp.zeros((CHIP, 64), F32)], axis=1)
                for t in range(5):
                    v = rj[:, t * 128:(t + 1) * 128]
                    Qf[t, pl.ds(row, ROWS), :] = v[0:ROWS]
                    Qs[t, (2 * p + j) * ROWS:(2 * p + j + 1) * ROWS, :] = v[ROWS:CHIP]
            q_send(p).start()
        for p in range(4):
            q_recv(p).wait_recv()
        for p in range(4):
            q_send(p).wait_send()

        def o_send(g2):
            r0 = g2 * 16
            return rdma(O16.at[:, pl.ds(r0, 16), :], O16.at[:, pl.ds(ROWS + r0, 16), :],
                        o_ss.at[g2], o_rs.at[g2], partner)

        for g in range(4):
            cp_kv(l, g).wait()
            if l == 0 and g > 0:
                for i in range(4):
                    cp_g(0, 4 * (g - 1) + i).start()
            sc = []
            for i in range(8):
                b = g * 8 + i
                qb = jnp.concatenate([Qf[t, pl.ds(b, HEADS, stride=ROWS), :] for t in range(5)], axis=1)
                s = jnp.dot(qb[:, 0:KV_W].astype(BF16), KV[b], preferred_element_type=F32) * QK_SCALE
                pos = lax.broadcasted_iota(jnp.int32, (HEADS, SEQ), 1)
                sc.append(jnp.where(pos < lens[b], s, -1e30))
            s = jnp.concatenate(sc, axis=0)
            e = jnp.exp(s - jnp.max(s, axis=-1, keepdims=True))
            pr = (e / jnp.sum(e, axis=-1, keepdims=True)).astype(BF16)
            for i in range(8):
                b = g * 8 + i
                o = lax.dot_general(pr[i * HEADS:(i + 1) * HEADS], KV[b, 0:LATENT, :], (((1,), (1,)), ((), ())),
                                    preferred_element_type=F32)
                for t in range(4):
                    Qf[t, pl.ds(b, HEADS, stride=ROWS), :] = o[:, t * 128:(t + 1) * 128]
            if g % 2 == 1:
                r0 = (g // 2) * 16
                for h in range(HEADS):
                    for t in range(4):
                        O16[h, r0:r0 + 16, t * 128:(t + 1) * 128] = (
                            Qf[t, h * ROWS + r0:h * ROWS + r0 + 16, :].astype(BF16))
                o_send(g // 2).start()
        for g2 in range(2):
            r0 = g2 * 16
            ref = O16.at[:, pl.ds(ROWS + r0, 16), :]
            rdma(ref, ref, o_ss.at[g2], o_rs.at[g2], partner).wait_recv()
        for g2 in range(2):
            o_send(g2).wait_send()

        for i in range(8):
            cp_wo(l, i).wait()
        if l == 0:
            for i in range(4):
                cp_d(0, i).start()
        for j in range(2):
            acc = None
            for k in range(8):
                for hh in range(2):
                    t = jnp.dot(O16[2 * k + hh], S[k, hh * LATENT:(hh + 1) * LATENT, j * NC:(j + 1) * NC],
                                preferred_element_type=F32)
                    acc = t if acc is None else acc + t
            n = own_n(j)
            X[n, pl.ds(my_row, ROWS), :] = (X[n, pl.ds(my_row, ROWS), :].astype(F32) + acc[0:ROWS]).astype(BF16)
            X[n, pl.ds(pa_row, ROWS), :] = (X[n, pl.ds(pa_row, ROWS), :].astype(F32) + acc[ROWS:CHIP]).astype(BF16)
            gather_start(j)
        if l + 1 == LAYERS:
            for i in range(8):
                cp_hs(i).start()

        def flip(k):
            w, j = k % 2, k // 2
            cp_g(l, k).wait()

            for row in range(j * NC, (j + 1) * NC, 256):
                for q in range(8):
                    G[w, row:row + 256, q * 256:(q + 1) * 256] = G[w, row:row + 256, q * 256:(q + 1) * 256].T

        def flips(a, b):
            def work():
                for k in range(a, b):
                    flip(k)
            return work

        gather_finish(flips(0, 5), flips(5, 8), flips(8, 10))

        for r in range(4):
            norm_to_h(r * ROWS, ROWS, r * ROWS, gf[l:l + 1, :])
        if l + 1 < LAYERS:
            for i in range(8):
                cp_wq(l + 1, i).start()
            for i in range(4):
                cp_kv(l + 1, i).start()
        for i in range(10, 12):
            cp_g(l, i).wait()

        def ffn_cols(n0, size):
            g_ = lax.dot_general(H[...], G[0, pl.ds(n0, size), :], (((1,), (1,)), ((), ())),
                                 preferred_element_type=F32)
            u_ = lax.dot_general(H[...], G[1, pl.ds(n0, size), :], (((1,), (1,)), ((), ())),
                                 preferred_element_type=F32)
            A[:, pl.ds(n0, size)] = (jax.nn.silu(g_) * u_).astype(BF16)

        def ffn_step(n, carry):
            for half in range(2):
                row = pl.multiple_of(n * NC + half * 256, 256)
                gu = []
                for w in range(2):
                    acc = None
                    for q in range(8):
                        t = jnp.dot(H[:, q * 256:(q + 1) * 256], G[w, pl.ds(row, 256), q * 256:(q + 1) * 256],
                                    preferred_element_type=F32)
                        acc = t if acc is None else acc + t
                    gu.append(acc)
                A[:, pl.ds(row, 256)] = (jax.nn.silu(gu[0]) * gu[1]).astype(BF16)
            return carry

        lax.fori_loop(0, 5, ffn_step, 0)
        ffn_cols(5 * NC, FFN - 5 * NC)
        if l + 1 < LAYERS:
            for i in range(12):
                cp_g(l + 1, i).start()
        else:
            for i in range(8):
                cp_hg(i).start()
            for i in range(4, 6):
                cp_hx(i).start()

        def ps(j):
            return rdma(PS.at[j], R1.at[j], p_ss.at[j], p_rs.at[j], partner)

        def cs(j):
            return rdma(CS.at[j, pl.ds(oth_row, CHIP), :], R2.at[j], c_ss.at[j], c_rs.at[j], other)

        def down(i):
            cp_d(l, i).wait()
            y = jnp.dot(A[...], DN[i], preferred_element_type=F32)
            if l + 1 < LAYERS:
                cp_d(l + 1, i).start()
            else:
                cp_hd(i).start()
                cp_hx(i).start()
            return y

        def chip_sum(j):
            ps(j).wait_recv()
            CS[j] = CS[j] + R1[j]
            cs(j).start()

        PS[0] = down(0)
        ps(0).start()
        CS[0] = down(1)
        PS[1] = down(2)
        ps(1).start()
        chip_sum(0)
        CS[1] = down(3)
        chip_sum(1)
        last = l + 1 == LAYERS
        for j in range(2):
            cs(j).wait_recv()
            n = own_n(j)
            xr = X[n, pl.ds(chip_row, CHIP), :].astype(F32)
            X[n, pl.ds(chip_row, CHIP), :] = (xr + (CS[j, pl.ds(chip_row, CHIP), :] + R2[j])).astype(BF16)
            if last:
                gather_start(j)
            else:
                ad(j, own_n(j)).start()
        for j in range(2):
            ps(j).wait_send()
            cs(j).wait_send()
        if last:
            gather_finish()
        else:
            for j in range(2):
                ad(j, par_n(j)).wait_recv()
            for j in range(2):
                ad(j, own_n(j)).wait_send()

    for r in range(4):
        norm_to_h(r * ROWS, ROWS, r * ROWS, gl[...])
    for i in range(8):
        cp_hs(i).wait()
        cp_hg(i).wait()
    for i in range(4):
        cp_hd(i).wait()
        cp_hx(i).wait()
    for i in range(4, 6):
        cp_hx(i).wait()


HB = 1024
RING = 2
BLOCKS = VOCAB // HB
HELD = 12
STREAM = BLOCKS - HELD


def head_body(H, S, G, DN, wh, out, W, OH, OS, w_sem, oh_sem, os_sem):
    def cp_w(t, slot, k):
        col = pl.multiple_of((HELD + t) * HB, HB)
        return pltpu.make_async_copy(wh.at[pl.ds(k * 1024, 1024), pl.ds(col, HB)], W.at[slot, k], w_sem.at[slot, k])

    def cp_out(buf, sem, block):
        col = pl.multiple_of(block * HB, HB)
        return pltpu.make_async_copy(buf, out.at[:, pl.ds(col, HB)], sem)

    for t in range(RING):
        for k in range(2):
            cp_w(t, t, k).start()

    def dot(a, b):
        return jnp.dot(a, b, preferred_element_type=F32)

    def stream(t):
        slot = lax.rem(t, RING)
        cp_w(t, slot, 0).wait()
        cp_w(t, slot, 1).wait()

        @pl.when(t >= 2)
        def _():
            cp_out(OS.at[slot], os_sem.at[slot], HELD + t).wait()

        for i in range(2):
            cols = slice(i * NC, (i + 1) * NC)
            OS[slot, :, cols] = dot(H[:, 0:1024], W[slot, 0, :, cols]) + dot(H[:, 1024:2048], W[slot, 1, :, cols])

        @pl.when(t + RING < STREAM)
        def _():
            cp_w(t + RING, slot, 0).start()
            cp_w(t + RING, slot, 1).start()

        cp_out(OS.at[slot], os_sem.at[slot], HELD + t).start()

    def held(t, *values):
        @pl.when(t >= 1)
        def _():
            cp_out(OH, oh_sem.at[0], t).wait()

        width = HB // len(values)
        for i, value in enumerate(values):
            OH[:, i * width:(i + 1) * width] = value()
        cp_out(OH, oh_sem.at[0], t).start()

    def seg_s(t, carry):
        held(t, *[lambda i=i: dot(H[:, 0:1024], S[2 * t, :, i * NC:(i + 1) * NC])
                  + dot(H[:, 1024:2048], S[2 * t + 1, :, i * NC:(i + 1) * NC]) for i in range(2)])
        stream(t)
        return carry

    def seg_g(t, carry):
        g, col = t // 2 - 2, lax.rem(t, 2) * HB
        held(t, *[lambda i=i: dot(H[...], G[g, 0:D, pl.ds(pl.multiple_of(col + i * NC, NC), NC)]) for i in range(2)])
        stream(t)
        return carry

    def seg_d(t, carry):
        held(t, *[lambda i=i: dot(H[...], DN[2 * (t - 8) + i, 0:D, :]) for i in range(2)])
        stream(t)
        return carry

    def seg_x(t, carry):
        def part(i):
            col = pl.multiple_of((t - 10) * HB + i * NC, NC)
            return (dot(H[:, 0:640], G[0, D:D + 640, pl.ds(col, NC)])
                    + dot(H[:, 640:1280], G[1, D:D + 640, pl.ds(col, NC)])
                    + dot(H[:, 1280:2048], DN[2 * (t - 10) + i, D:D + 768, :]))

        held(t, lambda: part(0), lambda: part(1))
        stream(t)
        return carry

    def seg_w(t, carry):
        stream(t)
        return carry

    lax.fori_loop(0, 4, seg_s, 0)
    lax.fori_loop(4, 8, seg_g, 0)
    lax.fori_loop(8, 10, seg_d, 0)
    lax.fori_loop(10, 12, seg_x, 0)
    lax.fori_loop(12, STREAM, seg_w, 0)
    cp_out(OH, oh_sem.at[0], HELD - 1).wait()
    for o in range(2):
        t = STREAM - 2 + o
        cp_out(OS.at[t % 2], os_sem.at[t % 2], HELD + t).wait()


def head_kernel(normed, s_buf, g_buf, d_buf, w_head):
    vm = pl.BlockSpec(memory_space=pltpu.VMEM)
    hb = pl.BlockSpec(memory_space=pl.ANY)
    dma = pltpu.SemaphoreType.DMA
    held = [pltpu.with_memory_space_constraint(a, pltpu.VMEM) for a in (normed, s_buf, g_buf, d_buf)]
    return pl.pallas_call(
        head_body,
        out_shape=jax.ShapeDtypeStruct((ALL, VOCAB), F32),
        in_specs=[vm] * 4 + [hb],
        out_specs=hb,
        scratch_shapes=[pltpu.VMEM((RING, 2, 1024, HB), BF16), pltpu.VMEM((ALL, HB), F32), pltpu.VMEM((2, ALL, HB), F32),
                        dma((RING, 2)), dma((1,)), dma((2,))],
        compiler_params=pltpu.CompilerParams(vmem_limit_bytes=13500000),
        name='head',
    )(*held, w_head)


def layers_kernel(hidden, lengths, kv_t, norm_attn, w_q, w_o, norm_ffn, wg_t, wu_t, w_down, norm_final, w_head):
    hb = pl.BlockSpec(memory_space=pl.ANY)
    dma = pltpu.SemaphoreType.DMA
    vm = pl.BlockSpec(memory_space=pltpu.VMEM)
    scratch = [
        pltpu.VMEM((ROWS, D), BF16), pltpu.SMEM((ROWS,), jnp.int32), pltpu.VMEM((2, D), F32), pltpu.VMEM((2, D), F32),
        pltpu.VMEM((1, D), F32), dma((5,)),
        pltpu.VMEM((ROWS, KV_W, SEQ), BF16),
        pltpu.VMEM((4, ALL, NC), BF16),
        pltpu.VMEM((5, HEADS * ROWS, 128), F32),
        pltpu.VMEM((5, 8 * ROWS, 128), F32),
        pltpu.VMEM((HEADS, CHIP, LATENT), BF16),
        pltpu.VMEM((ALL, FFN_PAD), BF16),
        pltpu.VMEM((2, ALL, NC), F32),
        pltpu.VMEM((2, ALL, NC), F32),
        pltpu.VMEM((2, ALL, NC), F32),
        pltpu.VMEM((2, CHIP, NC), F32),
        dma((8,)), dma((12,)), dma((4,)), dma((4,)),
        dma((4,)), dma((4,)), dma((2,)), dma((2,)),
        dma((2,)), dma((2,)), dma((2,)), dma((2,)), dma((2,)), dma((2,)),
        dma((2,)), dma((2,)), dma((2,)), dma((2,)), dma((1,)), dma((1,)), dma((6,)),
    ]
    return pl.pallas_call(
        body,
        out_shape=[pltpu.VMEM((ALL, D), BF16), pltpu.VMEM((8, 1024, PAIR), BF16), pltpu.VMEM((2, FFN, D), BF16),
                   pltpu.VMEM((4, FFN_PAD, NC), BF16)],
        in_specs=[hb] * 12,
        out_specs=[vm] * 4,
        scratch_shapes=scratch,
        compiler_params=pltpu.CompilerParams(collective_id=0, has_side_effects=True, vmem_limit_bytes=13500000),
        name='layers',
    )(hidden, lengths, norm_attn, norm_ffn, norm_final.reshape(1, D), kv_t, w_q, w_o, wg_t, wu_t, w_down, w_head)


def solution(mesh):
    row_axes = ('rep', 'dp')
    specs_in = (P(row_axes, None), P(row_axes), P(None, row_axes, None, None), P(), P(), P(), P(),
                P(None, None, 'dp'), P(None, None, 'dp'), P(None, 'dp', None), P(), P(None, 'dp'))

    def device_step(hidden, lengths, kv_cache, norm_attn, w_q, w_o, norm_ffn, w_gate, w_up, w_down, norm_final, w_head):
        held = layers_kernel(hidden, lengths, jnp.swapaxes(kv_cache, 2, 3), norm_attn, w_q, w_o, norm_ffn,
                               jnp.swapaxes(w_gate, 1, 2), jnp.swapaxes(w_up, 1, 2), w_down, norm_final, w_head)
        return head_kernel(*held, w_head)

    return jax.shard_map(device_step, mesh=mesh, in_specs=specs_in, out_specs=P('rep', 'dp'), check_vma=False)
```

```python
import functools

import jax
import jax.numpy as jnp
from jax import lax
from jax.experimental import pallas as pl
from jax.experimental.pallas import tpu as pltpu
from jax.sharding import PartitionSpec as P

F32 = jnp.float32
BF16 = jnp.bfloat16
MESH = pl.DeviceIdType.MESH

D = 2048
HEADS = 16
LATENT = 512
KV_W = 576
SEQ = 128
ROWS = 32
CHIP = 64
ALL = 128
FFN = 2736
FFN_PAD = 2816
NC = 512
QH = HEADS * KV_W // 2
PAIR = 2 * KV_W
VOCAB = 25600
QK_SCALE = 192 ** -0.5
NORM_EPS = 1e-6
LAYERS = 2


def _rows_norm(chunks, gain, dtype=BF16):
    ss = sum(jnp.sum(v * v, axis=-1, keepdims=True) for v in chunks)
    inv = lax.rsqrt(ss * (1.0 / D) + NORM_EPS)
    return [(v * inv * gain[:, i * NC:(i + 1) * NC]).astype(dtype) for i, v in enumerate(chunks)]


def body(hid_h, lens_h, ga_h, gf_h, gl_h, kv, wq, wo, wg, wu, wd, wh, H, S, G, DN,
         hid, lens, ga, gf, gl, in_sem, KV, X, Qf, Qs, O16, A, PS, CS, R1, R2,
         s_sem, g_sem, d_sem, kv_sem, q_ss, q_rs, o_ss, o_rs, ad_ss, ad_rs, al_ss, al_rs, af_ss, af_rs,
         p_ss, p_rs, c_ss, c_rs, h_ss, h_rs, x_sem):
    me = lax.axis_index('dp')
    c = lax.rem(me, 2)
    chip = me // 2
    partner = me + 1 - 2 * c
    other = lax.rem(me + 2, 4)
    my_row = pl.multiple_of(me * ROWS, ROWS)
    pa_row = pl.multiple_of(partner * ROWS, ROWS)
    chip_row = pl.multiple_of(chip * CHIP, CHIP)
    oth_row = pl.multiple_of((1 - chip) * CHIP, CHIP)

    def rdma(src, dst, ss, rs, dev):
        return pltpu.make_async_remote_copy(src_ref=src, dst_ref=dst, send_sem=ss, recv_sem=rs,
                                            device_id={'dp': dev}, device_id_type=MESH)

    def cp_wq(l, i):
        p, kk = i // 2, i % 2
        col = pl.multiple_of(c * QH + p * PAIR, 128)
        return pltpu.make_async_copy(wq.at[l, pl.ds(kk * 1024, 1024), pl.ds(col, PAIR)], S.at[i], s_sem.at[i])

    def cp_wo(l, i):
        col = pl.multiple_of(c * 1024, 128)
        return pltpu.make_async_copy(wo.at[l, pl.ds(i * 1024, 1024), pl.ds(col, 1024)],
                                     S.at[i, :, pl.ds(0, 1024)], s_sem.at[i])

    def cp_g(l, i):
        w, j = i % 2, i // 2
        src = wg if w == 0 else wu
        rows = NC if j < 5 else FFN - 5 * NC
        return pltpu.make_async_copy(src.at[l, pl.ds(j * NC, rows), :], G.at[w, pl.ds(j * NC, rows), :], g_sem.at[i])

    def dn_col(i):
        owner = 1 - c if i % 2 == 0 else c
        return 2 * owner + i // 2

    def cp_d(l, i):
        col = pl.multiple_of(dn_col(i) * NC, NC)
        return pltpu.make_async_copy(wd.at[l, :, pl.ds(col, NC)], DN.at[i, pl.ds(0, FFN), :], d_sem.at[i])

    def cp_kv(l, i):
        return pltpu.make_async_copy(kv.at[l, pl.ds(i * 8, 8)], KV.at[pl.ds(i * 8, 8)], kv_sem.at[i])

    def cp_hs(i):
        return pltpu.make_async_copy(wh.at[pl.ds((i % 2) * 1024, 1024), pl.ds((i // 2) * 1024, 1024)],
                                     S.at[i, :, pl.ds(0, 1024)], s_sem.at[i])

    def cp_hg(i):
        g, j = i // 4, i % 4
        return pltpu.make_async_copy(wh.at[pl.ds(j * 512, 512), pl.ds(4096 + g * D, D)],
                                     G.at[g, pl.ds(j * 512, 512), :], g_sem.at[i])

    def cp_hd(i):
        return pltpu.make_async_copy(wh.at[:, pl.ds(8192 + i * NC, NC)], DN.at[i, pl.ds(0, D), :], d_sem.at[i])

    def cp_hx(i):
        if i >= 4:
            g = i - 4
            return pltpu.make_async_copy(wh.at[pl.ds(g * 640, 640), pl.ds(10240, D)],
                                         G.at[g, pl.ds(D, 640), :], x_sem.at[i])
        return pltpu.make_async_copy(wh.at[pl.ds(1280, 768), pl.ds(10240 + i * NC, NC)],
                                     DN.at[i, pl.ds(D, 768), :], x_sem.at[i])

    ins = [pltpu.make_async_copy(a, b, in_sem.at[i]) for i, (a, b) in enumerate(
        ((hid_h, hid), (lens_h, lens), (ga_h, ga), (gf_h, gf), (gl_h, gl)))]
    for cp in ins:
        cp.start()
    for i in range(4):
        cp_wq(0, i).start()

    bar = pltpu.get_barrier_semaphore()
    for dev in (partner, other):
        pl.semaphore_signal(bar, inc=1, device_id={'dp': dev}, device_id_type=MESH)
    pl.semaphore_wait(bar, 2)

    ins[0].wait()
    for n in range(4):
        X[n, pl.ds(my_row, ROWS), :] = hid[:, n * NC:(n + 1) * NC]
    hx = rdma(X.at[:, pl.ds(my_row, ROWS), :], X.at[:, pl.ds(my_row, ROWS), :], h_ss.at[0], h_rs.at[0], partner)
    hx.start()
    for i in range(4):
        DN[i, FFN:FFN_PAD, :] = jnp.zeros((FFN_PAD - FFN, NC), BF16)
    A[:, FFN_PAD - 128:FFN_PAD] = jnp.zeros((ALL, 128), BF16)
    for cp in ins[1:]:
        cp.wait()
    hx.wait_send()
    rdma(X.at[:, pl.ds(pa_row, ROWS), :], X.at[:, pl.ds(pa_row, ROWS), :], h_ss.at[0], h_rs.at[0], partner).wait_recv()

    def x_chunks(row, rows):
        return [X[n, pl.ds(row, rows), :].astype(F32) for n in range(4)]

    def norm_to_h(row, rows, h_row, gain):
        for n, v in enumerate(_rows_norm(x_chunks(row, rows), gain)):
            H[pl.ds(h_row, rows), n * NC:(n + 1) * NC] = v

    def own_n(j):
        return 2 * c + j

    def par_n(j):
        return 2 * (1 - c) + j

    def ad(j, n):
        r = X.at[n, pl.ds(chip_row, CHIP), :]
        return rdma(r, r, ad_ss.at[j], ad_rs.at[j], partner)

    def al(j, row):
        r = X.at[own_n(j), pl.ds(row, CHIP), :]
        return rdma(r, r, al_ss.at[j], al_rs.at[j], other)

    def af(j, n):
        r = X.at[n, pl.ds(oth_row, CHIP), :]
        return rdma(r, r, af_ss.at[j], af_rs.at[j], partner)

    def gather_start(j):
        al(j, chip_row).start()
        ad(j, own_n(j)).start()

    def gather_finish(gain, *work):
        for j in range(2):
            if work:
                work[j]()
            al(j, oth_row).wait_recv()
            af(j, own_n(j)).start()
        if work:
            work[2]()
        for j in range(2):
            ad(j, par_n(j)).wait_recv()
        for r in range(2):
            row = pl.multiple_of(chip_row + r * ROWS, ROWS)
            norm_to_h(row, ROWS, row, gain)
        for j in range(2):
            af(j, par_n(j)).wait_recv()
        for r in range(2):
            row = pl.multiple_of(oth_row + r * ROWS, ROWS)
            norm_to_h(row, ROWS, row, gain)
        for j in range(2):
            al(j, chip_row).wait_send()
            ad(j, own_n(j)).wait_send()
            af(j, own_n(j)).wait_send()

    for l in range(LAYERS):
        norm_to_h(my_row, ROWS, 0, ga[l:l + 1, :])
        norm_to_h(pa_row, ROWS, ROWS, ga[l:l + 1, :])

        def q_send(p):
            dst = Qf.at[:, pl.ds(pl.multiple_of((c * 8 + 2 * p) * ROWS, ROWS), 2 * ROWS), :]
            return rdma(Qs.at[:, pl.ds(2 * p * ROWS, 2 * ROWS), :], dst, q_ss.at[p], q_rs.at[p], partner)

        def q_recv(p):
            dst = Qf.at[:, pl.ds(pl.multiple_of(((1 - c) * 8 + 2 * p) * ROWS, ROWS), 2 * ROWS), :]
            return rdma(dst, dst, q_ss.at[p], q_rs.at[p], partner)

        for p in range(4):
            cp_wq(l, 2 * p).wait()
            cp_wq(l, 2 * p + 1).wait()
            if l == 0:
                if p < 2:
                    cp_wq(0, 2 * p + 4).start()
                    cp_wq(0, 2 * p + 5).start()
                if p == 1:
                    for i in range(4):
                        cp_kv(0, i).start()
                if p == 2:
                    for i in range(4):
                        cp_wo(0, i).start()
            r = jnp.dot(H[0:CHIP, 0:1024], S[2 * p], preferred_element_type=F32)
            r = r + jnp.dot(H[0:CHIP, 1024:2048], S[2 * p + 1], preferred_element_type=F32)
            if l > 0 or p > 1:
                cp_wo(l, 2 * p).start()
                cp_wo(l, 2 * p + 1).start()
            r = r.astype(BF16).astype(F32)
            for j in range(2):
                rj = r[:, j * KV_W:(j + 1) * KV_W]
                row = pl.multiple_of((c * 8 + 2 * p + j) * ROWS, ROWS)
                rj = jnp.concatenate([rj, jnp.zeros((CHIP, 64), F32)], axis=1)
                for t in range(5):
                    v = rj[:, t * 128:(t + 1) * 128]
                    Qf[t, pl.ds(row, ROWS), :] = v[0:ROWS]
                    Qs[t, (2 * p + j) * ROWS:(2 * p + j + 1) * ROWS, :] = v[ROWS:CHIP]
            q_send(p).start()
        for p in range(4):
            q_recv(p).wait_recv()
        for p in range(4):
            q_send(p).wait_send()

        def o_send(g2):
            r0 = g2 * 16
            return rdma(O16.at[:, pl.ds(r0, 16), :], O16.at[:, pl.ds(ROWS + r0, 16), :],
                        o_ss.at[g2], o_rs.at[g2], partner)

        for g2 in range(2):
            prs = []
            for g in (2 * g2, 2 * g2 + 1):
                cp_kv(l, g).wait()
                if l == 0 and g > 0:
                    for i in range(4):
                        cp_g(0, 4 * (g - 1) + i).start()
            for g in (2 * g2, 2 * g2 + 1):
                sc = []
                for i in range(8):
                    b = g * 8 + i
                    qb = jnp.concatenate([Qf[t, pl.ds(b, HEADS, stride=ROWS), :] for t in range(5)], axis=1)
                    s = jnp.dot(qb[:, 0:KV_W].astype(BF16), KV[b], preferred_element_type=F32) * QK_SCALE
                    pos = lax.broadcasted_iota(jnp.int32, (HEADS, SEQ), 1)
                    sc.append(jnp.where(pos < lens[b], s, -1e30))
                s = jnp.concatenate(sc, axis=0)
                e = jnp.exp(s - jnp.max(s, axis=-1, keepdims=True))
                prs.append((e / jnp.sum(e, axis=-1, keepdims=True)).astype(BF16))
            for g in (2 * g2, 2 * g2 + 1):
                pr = prs[g % 2]
                for i in range(8):
                    b = g * 8 + i
                    o = lax.dot_general(pr[i * HEADS:(i + 1) * HEADS], KV[b, 0:LATENT, :], (((1,), (1,)), ((), ())),
                                        preferred_element_type=F32)
                    for t in range(4):
                        Qf[t, pl.ds(b, HEADS, stride=ROWS), :] = o[:, t * 128:(t + 1) * 128]
            r0 = g2 * 16
            for h in range(HEADS):
                for t in range(4):
                    O16[h, r0:r0 + 16, t * 128:(t + 1) * 128] = (
                        Qf[t, h * ROWS + r0:h * ROWS + r0 + 16, :].astype(BF16))
            o_send(g2).start()
        for g2 in range(2):
            r0 = g2 * 16
            ref = O16.at[:, pl.ds(ROWS + r0, 16), :]
            rdma(ref, ref, o_ss.at[g2], o_rs.at[g2], partner).wait_recv()
        for g2 in range(2):
            o_send(g2).wait_send()

        for i in range(8):
            cp_wo(l, i).wait()
        if l == 0:
            for i in range(4):
                cp_d(0, i).start()
        for j in range(2):
            acc = None
            for k in range(8):
                for hh in range(2):
                    t = jnp.dot(O16[2 * k + hh], S[k, hh * LATENT:(hh + 1) * LATENT, j * NC:(j + 1) * NC],
                                preferred_element_type=F32)
                    acc = t if acc is None else acc + t
            n = own_n(j)
            X[n, pl.ds(my_row, ROWS), :] = (X[n, pl.ds(my_row, ROWS), :].astype(F32) + acc[0:ROWS]).astype(BF16)
            X[n, pl.ds(pa_row, ROWS), :] = (X[n, pl.ds(pa_row, ROWS), :].astype(F32) + acc[ROWS:CHIP]).astype(BF16)
            gather_start(j)
        if l + 1 == LAYERS:
            for i in range(8):
                cp_hs(i).start()

        def flip(k):
            w, j = k % 2, k // 2
            cp_g(l, k).wait()

            for row in range(j * NC, (j + 1) * NC, 256):
                for q in range(8):
                    G[w, row:row + 256, q * 256:(q + 1) * 256] = G[w, row:row + 256, q * 256:(q + 1) * 256].T

        def flips(a, b):
            def work():
                for k in range(a, b):
                    flip(k)
            return work

        gather_finish(gf[l:l + 1, :], flips(0, 5), flips(5, 8), flips(8, 10))

        if l + 1 < LAYERS:
            for i in range(8):
                cp_wq(l + 1, i).start()
            for i in range(4):
                cp_kv(l + 1, i).start()
        for i in range(10, 12):
            cp_g(l, i).wait()

        def ffn_cols(n0, size):
            g_ = lax.dot_general(H[...], G[0, pl.ds(n0, size), :], (((1,), (1,)), ((), ())),
                                 preferred_element_type=F32)
            u_ = lax.dot_general(H[...], G[1, pl.ds(n0, size), :], (((1,), (1,)), ((), ())),
                                 preferred_element_type=F32)
            A[:, pl.ds(n0, size)] = (jax.nn.silu(g_) * u_).astype(BF16)

        def ffn_step(n, carry):
            for half in range(2):
                row = pl.multiple_of(n * NC + half * 256, 256)
                gu = []
                for w in range(2):
                    acc = None
                    for q in range(8):
                        t = jnp.dot(H[:, q * 256:(q + 1) * 256], G[w, pl.ds(row, 256), q * 256:(q + 1) * 256],
                                    preferred_element_type=F32)
                        acc = t if acc is None else acc + t
                    gu.append(acc)
                A[:, pl.ds(row, 256)] = (jax.nn.silu(gu[0]) * gu[1]).astype(BF16)
            return carry

        lax.fori_loop(0, 5, ffn_step, 0)
        ffn_cols(5 * NC, FFN - 5 * NC)
        if l + 1 < LAYERS:
            for i in range(12):
                cp_g(l + 1, i).start()
        else:
            for i in range(8):
                cp_hg(i).start()
            for i in range(4, 6):
                cp_hx(i).start()

        def ps(j):
            return rdma(PS.at[j], R1.at[j], p_ss.at[j], p_rs.at[j], partner)

        def cs(j):
            return rdma(CS.at[j, pl.ds(oth_row, CHIP), :], R2.at[j], c_ss.at[j], c_rs.at[j], other)

        def down(i):
            cp_d(l, i).wait()
            y = jnp.dot(A[...], DN[i], preferred_element_type=F32)
            if l + 1 < LAYERS:
                cp_d(l + 1, i).start()
            else:
                cp_hd(i).start()
                cp_hx(i).start()
            return y

        def chip_sum(j):
            ps(j).wait_recv()
            CS[j] = CS[j] + R1[j]
            cs(j).start()

        PS[0] = down(0)
        ps(0).start()
        CS[0] = down(1)
        PS[1] = down(2)
        ps(1).start()
        chip_sum(0)
        CS[1] = down(3)
        chip_sum(1)
        last = l + 1 == LAYERS
        for j in range(2):
            cs(j).wait_recv()
            n = own_n(j)
            xr = X[n, pl.ds(chip_row, CHIP), :].astype(F32)
            X[n, pl.ds(chip_row, CHIP), :] = (xr + (CS[j, pl.ds(chip_row, CHIP), :] + R2[j])).astype(BF16)
            if last:
                gather_start(j)
            else:
                ad(j, own_n(j)).start()
        for j in range(2):
            ps(j).wait_send()
            cs(j).wait_send()
        if last:
            gather_finish(gl[...])
        else:
            for j in range(2):
                ad(j, par_n(j)).wait_recv()
            for j in range(2):
                ad(j, own_n(j)).wait_send()

    for i in range(8):
        cp_hs(i).wait()
        cp_hg(i).wait()
    for i in range(4):
        cp_hd(i).wait()
        cp_hx(i).wait()
    for i in range(4, 6):
        cp_hx(i).wait()


HB = 1024
RING = 2
BLOCKS = VOCAB // HB
HELD = 12
STREAM = BLOCKS - HELD


def head_body(H, S, G, DN, wh, out, W, OH, OS, w_sem, oh_sem, os_sem):
    def cp_w(t, slot, k):
        col = pl.multiple_of((HELD + t) * HB, HB)
        return pltpu.make_async_copy(wh.at[pl.ds(k * 1024, 1024), pl.ds(col, HB)], W.at[slot, k], w_sem.at[slot, k])

    def cp_out(buf, sem, block):
        col = pl.multiple_of(block * HB, HB)
        return pltpu.make_async_copy(buf, out.at[:, pl.ds(col, HB)], sem)

    for t in range(RING):
        for k in range(2):
            cp_w(t, t, k).start()

    def dot(a, b):
        return jnp.dot(a, b, preferred_element_type=F32)

    def stream(t):
        slot = lax.rem(t, RING)
        cp_w(t, slot, 0).wait()
        cp_w(t, slot, 1).wait()

        @pl.when(t >= 2)
        def _():
            cp_out(OS.at[slot], os_sem.at[slot], HELD + t).wait()

        for i in range(2):
            cols = slice(i * NC, (i + 1) * NC)
            OS[slot, :, cols] = dot(H[:, 0:1024], W[slot, 0, :, cols]) + dot(H[:, 1024:2048], W[slot, 1, :, cols])

        @pl.when(t + RING < STREAM)
        def _():
            cp_w(t + RING, slot, 0).start()
            cp_w(t + RING, slot, 1).start()

        cp_out(OS.at[slot], os_sem.at[slot], HELD + t).start()

    def held(t, *values):
        @pl.when(t >= 1)
        def _():
            cp_out(OH, oh_sem.at[0], t).wait()

        width = HB // len(values)
        for i, value in enumerate(values):
            OH[:, i * width:(i + 1) * width] = value()
        cp_out(OH, oh_sem.at[0], t).start()

    def seg_s(t, carry):
        held(t, *[lambda i=i: dot(H[:, 0:1024], S[2 * t, :, i * NC:(i + 1) * NC])
                  + dot(H[:, 1024:2048], S[2 * t + 1, :, i * NC:(i + 1) * NC]) for i in range(2)])
        stream(t)
        return carry

    def seg_g(t, carry):
        g, col = t // 2 - 2, lax.rem(t, 2) * HB
        held(t, *[lambda i=i: dot(H[...], G[g, 0:D, pl.ds(pl.multiple_of(col + i * NC, NC), NC)]) for i in range(2)])
        stream(t)
        return carry

    def seg_d(t, carry):
        held(t, *[lambda i=i: dot(H[...], DN[2 * (t - 8) + i, 0:D, :]) for i in range(2)])
        stream(t)
        return carry

    def seg_x(t, carry):
        def part(i):
            col = pl.multiple_of((t - 10) * HB + i * NC, NC)
            return (dot(H[:, 0:640], G[0, D:D + 640, pl.ds(col, NC)])
                    + dot(H[:, 640:1280], G[1, D:D + 640, pl.ds(col, NC)])
                    + dot(H[:, 1280:2048], DN[2 * (t - 10) + i, D:D + 768, :]))

        held(t, lambda: part(0), lambda: part(1))
        stream(t)
        return carry

    def seg_w(t, carry):
        stream(t)
        return carry

    lax.fori_loop(0, 4, seg_s, 0)
    lax.fori_loop(4, 8, seg_g, 0)
    lax.fori_loop(8, 10, seg_d, 0)
    lax.fori_loop(10, 12, seg_x, 0)
    lax.fori_loop(12, STREAM, seg_w, 0)
    cp_out(OH, oh_sem.at[0], HELD - 1).wait()
    for o in range(2):
        t = STREAM - 2 + o
        cp_out(OS.at[t % 2], os_sem.at[t % 2], HELD + t).wait()


def head_kernel(normed, s_buf, g_buf, d_buf, w_head):
    vm = pl.BlockSpec(memory_space=pltpu.VMEM)
    hb = pl.BlockSpec(memory_space=pl.ANY)
    dma = pltpu.SemaphoreType.DMA
    held = [pltpu.with_memory_space_constraint(a, pltpu.VMEM) for a in (normed, s_buf, g_buf, d_buf)]
    return pl.pallas_call(
        head_body,
        out_shape=jax.ShapeDtypeStruct((ALL, VOCAB), F32),
        in_specs=[vm] * 4 + [hb],
        out_specs=hb,
        scratch_shapes=[pltpu.VMEM((RING, 2, 1024, HB), BF16), pltpu.VMEM((ALL, HB), F32), pltpu.VMEM((2, ALL, HB), F32),
                        dma((RING, 2)), dma((1,)), dma((2,))],
        compiler_params=pltpu.CompilerParams(vmem_limit_bytes=13500000),
        name='head',
    )(*held, w_head)


def layers_kernel(hidden, lengths, kv_t, norm_attn, w_q, w_o, norm_ffn, wg_t, wu_t, w_down, norm_final, w_head):
    hb = pl.BlockSpec(memory_space=pl.ANY)
    dma = pltpu.SemaphoreType.DMA
    vm = pl.BlockSpec(memory_space=pltpu.VMEM)
    scratch = [
        pltpu.VMEM((ROWS, D), BF16), pltpu.SMEM((ROWS,), jnp.int32), pltpu.VMEM((2, D), F32), pltpu.VMEM((2, D), F32),
        pltpu.VMEM((1, D), F32), dma((5,)),
        pltpu.VMEM((ROWS, KV_W, SEQ), BF16),
        pltpu.VMEM((4, ALL, NC), BF16),
        pltpu.VMEM((5, HEADS * ROWS, 128), F32),
        pltpu.VMEM((5, 8 * ROWS, 128), F32),
        pltpu.VMEM((HEADS, CHIP, LATENT), BF16),
        pltpu.VMEM((ALL, FFN_PAD), BF16),
        pltpu.VMEM((2, ALL, NC), F32),
        pltpu.VMEM((2, ALL, NC), F32),
        pltpu.VMEM((2, ALL, NC), F32),
        pltpu.VMEM((2, CHIP, NC), F32),
        dma((8,)), dma((12,)), dma((4,)), dma((4,)),
        dma((4,)), dma((4,)), dma((2,)), dma((2,)),
        dma((2,)), dma((2,)), dma((2,)), dma((2,)), dma((2,)), dma((2,)),
        dma((2,)), dma((2,)), dma((2,)), dma((2,)), dma((1,)), dma((1,)), dma((6,)),
    ]
    return pl.pallas_call(
        body,
        out_shape=[pltpu.VMEM((ALL, D), BF16), pltpu.VMEM((8, 1024, PAIR), BF16), pltpu.VMEM((2, FFN, D), BF16),
                   pltpu.VMEM((4, FFN_PAD, NC), BF16)],
        in_specs=[hb] * 12,
        out_specs=[vm] * 4,
        scratch_shapes=scratch,
        compiler_params=pltpu.CompilerParams(collective_id=0, has_side_effects=True, vmem_limit_bytes=13500000),
        name='layers',
    )(hidden, lengths, norm_attn, norm_ffn, norm_final.reshape(1, D), kv_t, w_q, w_o, wg_t, wu_t, w_down, w_head)


def solution(mesh):
    row_axes = ('rep', 'dp')
    specs_in = (P(row_axes, None), P(row_axes), P(None, row_axes, None, None), P(), P(), P(), P(),
                P(None, None, 'dp'), P(None, None, 'dp'), P(None, 'dp', None), P(), P(None, 'dp'))

    def device_step(hidden, lengths, kv_cache, norm_attn, w_q, w_o, norm_ffn, w_gate, w_up, w_down, norm_final, w_head):
        held = layers_kernel(hidden, lengths, jnp.swapaxes(kv_cache, 2, 3), norm_attn, w_q, w_o, norm_ffn,
                               jnp.swapaxes(w_gate, 1, 2), jnp.swapaxes(w_up, 1, 2), w_down, norm_final, w_head)
        return head_kernel(*held, w_head)

    return jax.shard_map(device_step, mesh=mesh, in_specs=specs_in, out_specs=P('rep', 'dp'), check_vma=False)
```
